256 devices in a mesh: gx: 8 (over y, core), gy: 4 (over x), gz: 8 (over z).
Axes of the slice: x: 4, y: 4, z: 8, core: 2. Of those that a mesh axis runs over, the one named last changes fastest.
Arguments:
- density: float32 [128, 64, 8192], P('gx', 'gy', 'gz'), may hold values from -19 to 19
Outputs:
- potential: float32 [128, 64, 8192], P('gx', 'gy', 'gz')
- coulomb: float32 [64, 64], replicated
The draws below stay inside these ranges and needn't reach their ends.
All inputs are finite; a program needn't handle non-finite values.
Results may differ from the reference program's by a relative error of at most 0.000057.
Values sent between devices are 32-bit elements; how exact they have to be, the bound alone decides.
A program may use at most 64 MiB of HBM per device.

```python
import jax
import jax.numpy as jnp
from jax import lax

PAIRS = 64
LEVELS = 6
COARSE_SWEEPS = 8
NX = 128
NY = 64
NZ = 128


def draw_density(key, part):
    first, second = jax.random.split(jax.random.fold_in(key, 11), 2)
    noise = jnp.clip(jax.random.normal(first, (NX, NY, NZ, PAIRS), jnp.float32), -6.0, 6.0)
    offset = jax.random.uniform(second, (PAIRS,), jnp.float32, -0.02, 0.02)
    ramp = 1.0 + 2.0 * jnp.arange(NX, dtype=jnp.float32) / (NX - 1)
    values = (noise + offset) * ramp[:, None, None, None]
    return values.reshape(NX, NY, NZ * PAIRS)


def setup_inputs(seed: int = 0) -> dict:
    seeds = jax.random.split(jax.random.key(seed), 2)
    return {
        "density": draw_density(jax.random.fold_in(seeds[1], 71), 0),
    }


OMEGA = 2.0 / 3.0


def neighbours(padded):
    total = padded[2:, 1:-1, 1:-1] + padded[:-2, 1:-1, 1:-1]
    total = total + padded[1:-1, 2:, 1:-1] + padded[1:-1, :-2, 1:-1]
    return total + padded[1:-1, 1:-1, 2:] + padded[1:-1, 1:-1, :-2]


def apply_inner(padded, factor):
    return factor * (6.0 * padded[1:-1, 1:-1, 1:-1] - neighbours(padded))


def sweep_inner(padded, source, factor):
    return padded[1:-1, 1:-1, 1:-1] + OMEGA * (source - apply_inner(padded, factor)) / (6.0 * factor)


def zero_rim(current):
    return jnp.pad(current, ((1, 1), (1, 1), (1, 1), (0, 0)))


def restrict(residual):
    size_x, size_y, size_z, count = residual.shape
    grouped = residual.reshape(size_x // 2, 2, size_y // 2, 2, size_z // 2, 2, count)
    return jnp.mean(grouped, axis=(1, 3, 5))


def prolong(correction):
    return jnp.repeat(jnp.repeat(jnp.repeat(correction, 2, axis=0), 2, axis=1), 2, axis=2)


def cycle(source, grid_level):
    factor = 0.25 ** (grid_level - 1)
    current = OMEGA * source / (6.0 * factor)
    if grid_level == LEVELS:
        for repeat_no in range(COARSE_SWEEPS - 1):
            current = sweep_inner(zero_rim(current), source, factor)
        return current
    current = sweep_inner(zero_rim(current), source, factor)
    residual = source - apply_inner(zero_rim(current), factor)
    current = current + prolong(cycle(restrict(residual), grid_level + 1))
    for repeat_no in range(2):
        current = sweep_inner(zero_rim(current), source, factor)
    return current


def reference(density):
    cells = density.reshape(NX, NY, NZ, PAIRS)
    solved = cycle(cells, 1)
    block = jnp.dot(cells.reshape(-1, PAIRS).T, solved.reshape(-1, PAIRS), precision=lax.Precision.HIGHEST, preferred_element_type=jnp.float32)
    coulomb = block * (4.0 / (NX * NY * NZ))
    return solved.reshape(NX, NY, NZ * PAIRS), coulomb
```

```python
import functools

import jax
import jax.numpy as jnp
from jax import lax
from jax.experimental import pallas as pl
from jax.experimental.pallas import tpu as pltpu
from jax.sharding import PartitionSpec as P

PAIRS = 64
LANES = 128
YO = 8
CENTRE = 1.0 / 3.0
SIDE = 1.0 / 9.0
MESH = pl.DeviceIdType.MESH
F32 = jnp.float32


def tau(level):
    return (1.0 / 9.0) * 4.0 ** (level - 1)


def low_lanes():
    return lax.broadcasted_iota(jnp.int32, (1, LANES), 1) < PAIRS


def swap(v):
    return pltpu.roll(v, PAIRS, v.ndim - 1)


def smooth(a, t, x, row, n):
    own = a[t, x, pl.ds(row, n), :]
    total = a[t, x, pl.ds(row - 1, n), :] + a[t, x, pl.ds(row + 1, n), :]
    total = total + (a[t, x - 1, pl.ds(row, n), :] + a[t, x + 1, pl.ds(row, n), :])
    beyond = jnp.where(low_lanes(), a[t + 1, x, pl.ds(row, n), :], a[t - 1, x, pl.ds(row, n), :])
    total = total + swap(own + beyond)
    return own * CENTRE + total * SIDE


def loop(n, body, unroll_below=3):
    if n < unroll_below:
        for i in range(n):
            body(i)
    else:
        lax.fori_loop(0, n, lambda i, c: (body(i), c)[1], 0)


def restrict_rows(r, t, x, rows):
    s = r[t, x, pl.ds(YO, rows, stride=2), :] + r[t, x, pl.ds(YO + 1, rows, stride=2), :]
    s = s + (r[t, x + 1, pl.ds(YO, rows, stride=2), :] + r[t, x + 1, pl.ds(YO + 1, rows, stride=2), :])
    return s + swap(s)


def coarse_cell(r, tc, xc, rows):
    even = restrict_rows(r, 2 * tc + 1, 2 * xc + 1, rows)
    odd = restrict_rows(r, 2 * tc + 2, 2 * xc + 1, rows)
    return jnp.where(low_lanes(), even, odd) * 0.125


def zero_faces(a, tiles, planes, rows, inside=None):
    flat = jnp.zeros((rows, LANES), F32)
    line = jnp.zeros((1, LANES), F32)

    def plane(x):
        def body(t):
            a[t + 1, x, pl.ds(YO, rows), :] = flat

        return lambda: loop(tiles, body)

    def edge(row):
        def body(t):
            for x in range(1, planes + 1):
                a[t + 1, x, pl.ds(row, 1), :] = line

        return lambda: loop(tiles, body)

    def tile(t):
        def fill():
            for x in range(1, planes + 1):
                a[t, x, pl.ds(YO, rows), :] = flat

        return fill

    fills = (plane(0), plane(planes + 1), edge(YO - 1), edge(YO + rows), tile(0), tile(tiles + 1))
    for i, fill in enumerate(fills):
        if inside is None:
            fill()
        else:
            pl.when(jnp.logical_not(inside[i]))(fill)


def dot_t(a, b):
    return lax.dot_general(
        a, b, (((0,), (0,)), ((), ())), precision=lax.Precision.HIGHEST, preferred_element_type=F32
    )


def kernel(
    nums, dens, pot, coul,
    f1, h1, r1, w1, f2, h2, r2, w2, f3, h3, r3, w3,
    f4, h4, r4, q4, k4, c4, f5, h5, r5, q5, k5, c5, f6, a6, b6,
    q3, k3, c3, q2, k2, c2, q1, k1, out,
    acc, acc4, cp, ca, cs, cb, ct, cc,
    send, recv, io,
):
    ngx, ngy, ngz = nums
    gx, gy, gz = (lax.axis_index(a) for a in ("gx", "gy", "gz"))
    me = (gx, gy, gz)
    sizes = (ngx, ngy, ngz)
    names = ("gx", "gy", "gz")
    chip, core = gx // 2, gx % 2
    chips = ngx // 2
    counter = [0]
    sent = []

    def has(offset):
        cond = None
        for pos, size, d in zip(me, sizes, offset):
            if d == 0:
                continue
            this = pos + d >= 0 if d < 0 else pos + d < size
            cond = this if cond is None else cond & this
        return cond

    def when(cond, fn):
        if cond is None:
            fn()
        else:
            pl.when(cond)(fn)

    def opposite(offset):
        return tuple(-d for d in offset)

    def near(offset):
        return {n: p + d for n, p, d in zip(names, me, offset) if d != 0}

    class Msg:
        def __init__(self, src, dst, device, cond_send, cond_recv):
            i = counter[0]
            counter[0] += 1
            self.copy = pltpu.make_async_remote_copy(
                src_ref=src, dst_ref=dst, send_sem=send.at[i], recv_sem=recv.at[i], device_id=device, device_id_type=MESH
            )
            self.cond_send, self.cond_recv = cond_send, cond_recv

        def start(self):
            when(self.cond_send, self.copy.start)
            sent.append(self)

        def wait(self):
            when(self.cond_recv, self.copy.wait_recv)

        def drain(self):
            when(self.cond_send, self.copy.wait_send)

    def start(msgs):
        for m in msgs:
            m.start()
        return msgs

    def wait(msgs):
        for m in msgs:
            m.wait()

    def faces(a, tiles, planes, rows):
        ts, xs, ys = pl.ds(1, tiles), pl.ds(1, planes), pl.ds(YO, rows)
        spec = [
            ((-1, 0, 0), (ts, pl.ds(1, 1), ys), (ts, pl.ds(planes + 1, 1), ys)),
            ((1, 0, 0), (ts, pl.ds(planes, 1), ys), (ts, pl.ds(0, 1), ys)),
            ((0, -1, 0), (ts, xs, pl.ds(YO, 1)), (ts, xs, pl.ds(YO + rows, 1))),
            ((0, 1, 0), (ts, xs, pl.ds(YO + rows - 1, 1)), (ts, xs, pl.ds(YO - 1, 1))),
            ((0, 0, -1), (pl.ds(1, 1), xs, ys), (pl.ds(tiles + 1, 1), xs, ys)),
            ((0, 0, 1), (pl.ds(tiles, 1), xs, ys), (pl.ds(0, 1), xs, ys)),
        ]
        return start(
            [Msg(a.at[src], a.at[dst], near(o), has(o), has(opposite(o))) for o, src, dst in spec]
        )

    def rims(a, tiles, planes, rows, width, corners):
        def part(d, size, w, first):
            if d == 0:
                return pl.ds(first, size), pl.ds(first, size)
            if d < 0:
                return pl.ds(first, w), pl.ds(first + size, w)
            return pl.ds(first + size - w, w), pl.ds(first - w, w)

        msgs = []
        for dx in (-1, 0, 1):
            for dy in (-1, 0, 1):
                for dz in (-1, 0, 1):
                    order = abs(dx) + abs(dy) + abs(dz)
                    if order == 0 or (order == 3 and not corners):
                        continue
                    o = (dx, dy, dz)
                    z_src, z_dst = part(dz, tiles, 1, 1)
                    x_src, x_dst = part(dx, planes, width, width)
                    y_src, y_dst = part(dy, rows, width, width)
                    msgs.append(
                        (order, Msg(a.at[z_src, x_src, y_src], a.at[z_dst, x_dst, y_dst], near(o), has(o), has(opposite(o))))
                    )
        msgs.sort(key=lambda m: -m[0])
        return start([m for _, m in msgs])

    loads = [
        pltpu.make_async_copy(
            dens.at[:, :, pl.ds(t * LANES, LANES)], f1.at[t + 1, pl.ds(1, 16), pl.ds(YO, 16)], io.at[t]
        )
        for t in range(8)
    ]
    for c in loads:
        c.start()
    w2[...] = jnp.zeros(w2.shape, F32)
    w3[...] = jnp.zeros(w3.shape, F32)
    barrier = pltpu.get_barrier_semaphore()
    expected = jnp.int32(0)
    for dx in (-1, 0, 1):
        for dy in (-1, 0, 1):
            for dz in (-1, 0, 1):
                o = (dx, dy, dz)
                if o == (0, 0, 0):
                    continue
                cond = has(o)

                @pl.when(cond)
                def _(o=o):
                    pl.semaphore_signal(barrier, inc=1, device_id=near(o), device_id_type=MESH)

                expected = expected + cond.astype(jnp.int32)
    for d in range(1, ngz):
        pl.semaphore_signal(barrier, inc=1, device_id={"gz": lax.rem(gz + d, ngz)}, device_id_type=MESH)
    others = [(dx, dy) for dx in range(ngx) for dy in range(ngy) if (dx, dy) != (0, 0)]

    def other(dx, dy):
        return {"gx": lax.rem(gx + dx, ngx), "gy": lax.rem(gy + dy, ngy)}

    for dx, dy in others:
        pl.semaphore_signal(barrier, inc=1, device_id=other(dx, dy), device_id_type=MESH)
    expected = expected + (ngz - 1 + len(others))

    near_side = [has(o) for o in ((-1, 0, 0), (1, 0, 0), (0, -1, 0), (0, 1, 0), (0, 0, -1), (0, 0, 1))]
    for a in (f1, h1, r1):
        zero_faces(a, 8, 16, 16, near_side)
    for a in (f2, h2, r2):
        zero_faces(a, 4, 8, 8, near_side)
    for a in (f3, h3, r3):
        zero_faces(a, 2, 4, 4, near_side)
    x4, y4, t4 = 2 * ngx, 2 * ngy, ngz
    for a in (f4, h4, r4, q4, k4):
        zero_faces(a, t4, x4, y4)
    c4[...] = jnp.zeros(c4.shape, F32)
    for a in (f5, h5, r5, q5, k5):
        zero_faces(a, t4 // 2, x4 // 2, y4 // 2)
    for a in (f6, a6, b6):
        zero_faces(a, t4 // 4, x4 // 4, y4 // 4)
    acc[...] = jnp.zeros(acc.shape, F32)
    acc4[...] = jnp.zeros(acc4.shape, F32)

    for c in loads:
        c.wait()
    pl.semaphore_wait(barrier, expected)

    def apply(dst, src, tiles, planes, rows):
        def body(t):
            for x in range(1, planes + 1):
                dst[t + 1, x, pl.ds(YO, rows), :] = smooth(src, t + 1, x, YO, rows)

        loop(tiles, body)

    def restrict(dst, r, tiles, planes, rows):
        def body(tc):
            for xc in range(planes):
                dst[tc + 1, xc + 1, pl.ds(YO, rows), :] = coarse_cell(r, tc, xc, rows)

        loop(tiles, body)

    def collect(w, f, h, r, tiles, planes, rows, x0, y0, level):
        def body(t):
            for x in range(planes):
                at = (t + 1, x + 1, pl.ds(YO, rows), slice(None))
                v = f[at] + h[at] + r[at] + smooth(r, t + 1, x + 1, YO, rows)
                w[t + (x0 > 0), x + x0, pl.ds(y0, rows), :] = v * tau(level)

        loop(tiles, body)

    def energy(f, h, r, tiles, planes, rows, level):
        padded = -(-rows // 8) * 8
        keep = lax.broadcasted_iota(jnp.int32, (1, padded, 1), 1) < rows

        def body(t):
            at = (t + 1, pl.ds(1, planes), pl.ds(YO, padded), slice(None))
            vf, vh, vr = f[at], h[at], r[at]
            if padded != rows:
                vf, vh, vr = (jnp.where(keep, v, 0.0) for v in (vf, vh, vr))
            vf, vh, vr = (v.reshape(planes * padded, LANES) for v in (vf, vh, vr))
            acc[...] += (dot_t(vf, vf + vh) + dot_t(vh, vh + vr)) * (tau(level) * 8.0 ** (level - 1))

        loop(tiles, body)

    wait(faces(f1, 8, 16, 16))
    apply(h1, f1, 8, 16, 16)
    wait(faces(h1, 8, 16, 16))
    apply(r1, h1, 8, 16, 16)
    restrict(f2, r1, 4, 8, 8)
    m_f2 = faces(f2, 4, 8, 8)
    m_r1 = faces(r1, 8, 16, 16)
    energy(f1, h1, r1, 8, 16, 16, 1)
    wait(m_f2)
    apply(h2, f2, 4, 8, 8)
    m_h2 = faces(h2, 4, 8, 8)
    wait(m_r1)
    collect(w1, f1, h1, r1, 8, 16, 16, 0, 0, 1)
    wait(m_h2)
    apply(r2, h2, 4, 8, 8)
    restrict(f3, r2, 2, 4, 4)
    m_f3 = faces(f3, 2, 4, 4)
    m_r2 = faces(r2, 4, 8, 8)
    energy(f2, h2, r2, 4, 8, 8, 2)
    wait(m_f3)
    apply(h3, f3, 2, 4, 4)
    m_h3 = faces(h3, 2, 4, 4)
    wait(m_r2)
    collect(w2, f2, h2, r2, 4, 8, 8, 1, 1, 2)
    wait(m_h3)
    apply(r3, h3, 2, 4, 4)

    own_x, own_y = pl.ds(2 * gx + 1, 2), pl.ds(YO + 2 * gy, 2)
    for x in range(2):
        f4[gz + 1, 2 * gx + 1 + x, own_y, :] = coarse_cell(r3, 0, x, 2)
    all_t = pl.ds(1, t4)
    block = f4.at[pl.ds(gz + 1, 1), own_x, own_y]
    m_z = start(
        [Msg(block, block, {"gz": lax.rem(gz + d, ngz)}, None, None) for d in range(1, ngz)]
    )
    m_r3 = faces(r3, 2, 4, 4)
    m_w2 = rims(w2, 4, 8, 8, 1, False)
    wait(m_r3)
    energy(f3, h3, r3, 2, 4, 4, 3)
    collect(w3, f3, h3, r3, 2, 4, 4, 2, 2, 3)
    m_w3 = rims(w3, 2, 4, 4, 2, True)
    piece = 32 // ngz
    square = acc[0:PAIRS, :] + swap(acc[PAIRS:, :])
    packed = jnp.where(low_lanes(), square[0:32, :], swap(square[32:64, :]))
    for k in range(ngz):
        cp[k] = packed[k * piece : (k + 1) * piece, :]
    m_ca = []
    for d in range(1, ngz):
        to = lax.rem(gz + d, ngz)
        m_ca.append(Msg(cp.at[to], ca.at[gz], {"gz": to}, None, None))
    start(m_ca)
    ca[gz] = cp[gz]

    wait(m_z)
    line = f4.at[all_t, own_x, own_y]
    m_p = []
    for dx in range(chips):
        for dy in range(ngy):
            if (dx, dy) != (0, 0):
                to = {"gx": lax.rem(chip + dx, chips) * 2 + core, "gy": lax.rem(gy + dy, ngy)}
                m_p.append(Msg(line, line, to, None, None))
    start(m_p)
    wait(m_ca)
    total = ca[0]
    for k in range(1, ngz):
        total = total + ca[k]
    cs[...] = total
    slot = gx * ngy + gy
    cb[slot] = total
    m_cb = start([Msg(cs, cb.at[slot], other(dx, dy), None, None) for dx, dy in others])
    wait(m_p)
    m_c = []
    for j in range(chips):
        part = f4.at[all_t, pl.ds(2 * (2 * j + core) + 1, 2), pl.ds(YO, y4)]
        m_c.append(Msg(part, part, {"gx": 2 * chip + 1 - core}, None, None))
    start(m_c)
    wait(m_c)

    apply(h4, f4, t4, x4, y4)
    apply(r4, h4, t4, x4, y4)
    x5, y5, t5 = x4 // 2, y4 // 2, t4 // 2
    x6, y6, t6 = x5 // 2, y5 // 2, t5 // 2
    restrict(f5, r4, t5, x5, y5)
    apply(h5, f5, t5, x5, y5)
    apply(r5, h5, t5, x5, y5)
    restrict(f6, r5, t6, x6, y6)
    for t in range(1, t6 + 1):
        for x in range(1, x6 + 1):
            at = (t, x, pl.ds(YO, y6), slice(None))
            v = f6[at] * tau(6)
            f6[at] = v
            a6[at] = v
    now, later = a6, b6
    for _ in range(7):
        for t in range(1, t6 + 1):
            for x in range(1, x6 + 1):
                at = (t, x, pl.ds(YO, y6), slice(None))
                later[at] = f6[at] + smooth(now, t, x, YO, y6)
        now, later = later, now

    def prolong(dst, value, tile, x, row, rows, which=(0, 1)):
        turned = swap(value)
        halves = (jnp.where(low_lanes(), value, turned), jnp.where(low_lanes(), turned, value))
        for k in which:
            for i in range(2):
                for j in range(2):
                    dst[tile + k, x + i, pl.ds(row + j, rows, stride=2), :] = halves[k]

    def coarse_up(c, f, h, r, q, k, coarse, first, tiles, planes, rows, level, pad):
        def spread(t):
            for x in range(planes // 2):
                value = coarse[t + 1, x + first, pl.ds(YO, rows // 2), :]
                prolong(q, value, 2 * t + 1, 2 * x + 1, YO, rows // 2)

        loop(tiles // 2, spread)
        apply(k, q, tiles, planes, rows)

        def body(t):
            for x in range(1, planes + 1):
                at = (t + 1, x, pl.ds(YO, rows), slice(None))
                v = (f[at] + h[at] + r[at] + smooth(r, t + 1, x, YO, rows)) * tau(level)
                c[t + 1, x + pad, pl.ds(YO, rows), :] = v + smooth(k, t + 1, x, YO, rows)

        loop(tiles, body)

    coarse_up(c5, f5, h5, r5, q5, k5, now, 1, t5, x5, y5, 5, 0)
    coarse_up(c4, f4, h4, r4, q4, k4, c5, 1, t4, x4, y4, 4, 1)

    wait(m_cb)
    total = cb[0]
    for k in range(1, ngx * ngy):
        total = total + cb[k]
    ct[...] = total
    cc[gz] = total
    m_cc = start(
        [Msg(ct, cc.at[gz], {"gz": lax.rem(gz + d, ngz)}, None, None) for d in range(1, ngz)]
    )

    inside = [
        tuple(c.astype(F32) for c in (p > 0, p < n - 1)) for p, n in zip(me, sizes)
    ]

    def row_mask(n, first, own):
        row = lax.broadcasted_iota(jnp.int32, (n, LANES), 0)
        one = jnp.ones((n, LANES), F32)
        return jnp.where(row < first, one * inside[1][0], jnp.where(row >= first + own, one * inside[1][1], one))

    def side(axis, i, own):
        return inside[axis][0] if i < 0 else inside[axis][1] if i >= own else None

    def masked(v, mask, *scalars):
        v = v * mask
        for s in scalars:
            if s is not None:
                v = v * s
        return v

    wait(m_w3)
    for j in range(3):
        for i in range(6):
            value = c4[gz + j, 2 * gx + i, pl.ds(YO - 2 + 2 * gy, 6), :]
            prolong(q3, value, 1 + 2 * j, 2 * i, 0, 6)
    mask = row_mask(10, 3, 4)
    for t in range(-2, 4):
        for x in range(-3, 7):
            v = smooth(q3, t + 3, x + 4, 1, 10)
            k3[t + 3, x + 4, pl.ds(1, 10), :] = masked(v, mask, side(2, t, 2), side(0, x, 4))
    mask = row_mask(8, 2, 4)
    for t in range(-1, 3):
        for x in range(-2, 6):
            v = w3[t + 1, x + 2, pl.ds(0, 8), :] + smooth(k3, t + 3, x + 4, 2, 8)
            prolong(q2, masked(v, mask, side(2, t, 2), side(0, x, 4)), 2 * t + 3, 2 * x + 4, 0, 8)

    wait(m_w2)
    mask = row_mask(12, 2, 8)
    for t in range(-1, 5):
        for x in range(-2, 10):
            v = smooth(q2, t + 3, x + 4, 2, 12)
            k2[t + 3, x + 4, pl.ds(2, 12), :] = masked(v, mask, side(2, t, 4), side(0, x, 8))
    mask = row_mask(10, 1, 8)
    for t in range(-1, 5):
        for x in range(-1, 9):
            v = w2[t + 1, x + 1, pl.ds(0, 10), :] + smooth(k2, t + 3, x + 4, 3, 10)
            which = (1,) if t < 0 else (0,) if t >= 4 else (0, 1)
            prolong(q1, masked(v, mask, side(2, t, 4), side(0, x, 8)), 2 * t + 2, 2 * x + 2, 0, 10, which)

    mask = row_mask(18, 1, 16)

    def rim_tile(t):
        for x in range(0, 16):
            v = smooth(q1, t + 2, x + 2, 1, 18)
            k1[t + 2, x + 2, pl.ds(1, 18), :] = masked(v, mask, side(2, t, 8))

    def own_tile(t):
        for x in range(-1, 17):
            v = smooth(q1, t + 2, x + 2, 1, 18)
            k1[t + 2, x + 2, pl.ds(1, 18), :] = masked(v, mask, side(0, x, 16))

    rim_tile(-1)
    rim_tile(8)
    loop(8, own_tile)

    def last(t):
        for x in range(16):
            out[t, x] = w1[t, x] + smooth(k1, t + 2, x + 2, 2, 16)

    loop(8, last)
    stores = [
        pltpu.make_async_copy(out.at[t], pot.at[:, :, pl.ds(t * LANES, LANES)], io.at[t]) for t in range(8)
    ]
    for c in stores:
        c.start()

    padded = -(-y4 // 8) * 8
    keep = lax.broadcasted_iota(jnp.int32, (1, padded, 1), 1) < y4

    def level_4(t):
        vf = f4[t + 1, pl.ds(1, x4), pl.ds(YO, padded), :]
        vc = c4[t + 1, pl.ds(2, x4), pl.ds(YO, padded), :]
        if padded != y4:
            vf, vc = (jnp.where(keep, v, 0.0) for v in (vf, vc))
        acc4[...] += dot_t(vf.reshape(x4 * padded, LANES), vc.reshape(x4 * padded, LANES))

    loop(t4, level_4)
    coarse_part = (acc4[0:PAIRS, :] + swap(acc4[PAIRS:, :])) * 512.0
    wait(m_cc)
    packed = jnp.concatenate([cc[k] for k in range(ngz)], axis=0)
    scale = 4.0 / (ngx * ngy * ngz * 16 * 16 * 16)
    coul[0:32, :] = ((packed + coarse_part[0:32, :]) * scale)[:, :PAIRS]
    coul[32:64, :] = ((swap(packed) + coarse_part[32:64, :]) * scale)[:, :PAIRS]

    for c in stores:
        c.wait()
    for m in sent:
        m.drain()


def local(nums, density):
    ngx, ngy, ngz = nums
    piece = 32 // ngz

    def field(t, x, y):
        return pltpu.VMEM((t, x, y, LANES), F32)

    def level(t, x, y):
        return field(t + 2, x + 2, YO + -(-(y + 1) // 8) * 8)

    t4, x4, y4 = ngz, 2 * ngx, 2 * ngy
    l1, l2, l3 = level(8, 16, 16), level(4, 8, 8), level(2, 4, 4)
    l4, l5, l6 = (level(t4 // s, x4 // s, y4 // s) for s in (1, 2, 4))
    c4 = field(t4 + 2, x4 + 4, 24)
    scratch = [l1, l1, l1, field(8, 16, 16), l2, l2, l2, field(6, 10, 16), l3, l3, l3, field(4, 8, 8)]
    scratch += [l4, l4, l4, l4, l4, c4, l5, l5, l5, l5, l5, l5, l6, l6, l6]
    scratch += [field(8, 12, 16), field(8, 12, 16), field(1, 1, 8), field(10, 16, 16), field(10, 16, 16), field(1, 1, 8)]
    scratch += [field(12, 20, 24), field(12, 20, 24), field(8, 16, 16)]
    square = pltpu.VMEM((LANES, LANES), F32)
    row = pltpu.VMEM((piece, LANES), F32)
    scratch += [square, square, pltpu.VMEM((ngz, piece, LANES), F32), pltpu.VMEM((ngz, piece, LANES), F32), row]
    scratch += [pltpu.VMEM((ngx * ngy, piece, LANES), F32), row, pltpu.VMEM((ngz, piece, LANES), F32)]
    messages = 54 + 18 + 26 + 3 * (ngz - 1) + (ngx // 2 * ngy - 1) + (ngx * ngy - 1) + ngx // 2
    scratch += [pltpu.SemaphoreType.DMA((messages,)), pltpu.SemaphoreType.DMA((messages,)), pltpu.SemaphoreType.DMA((8,))]
    return pl.pallas_call(
        functools.partial(kernel, nums),
        out_shape=(
            jax.ShapeDtypeStruct(density.shape, F32),
            jax.ShapeDtypeStruct((PAIRS, PAIRS), F32),
        ),
        in_specs=[pl.BlockSpec(memory_space=pl.ANY)],
        out_specs=(pl.BlockSpec(memory_space=pl.ANY), pl.BlockSpec(memory_space=pltpu.VMEM)),
        scratch_shapes=scratch,
        compiler_params=pltpu.CompilerParams(
            collective_id=0, has_side_effects=True, vmem_limit_bytes=60_000_000
        ),
        name="cycle",
    )(density)


def solution(mesh):
    nums = tuple(mesh.shape[a] for a in ("gx", "gy", "gz"))
    placed = P("gx", "gy", "gz")
    return jax.shard_map(
        functools.partial(local, nums), mesh=mesh, in_specs=(placed,), out_specs=(placed, P()), check_vma=False
    )
```

```python
import functools

import jax
import jax.numpy as jnp
from jax import lax
from jax.experimental import pallas as pl
from jax.experimental.pallas import tpu as pltpu
from jax.sharding import PartitionSpec as P

PAIRS = 64
LANES = 128
YO = 8
CENTRE = 1.0 / 3.0
SIDE = 1.0 / 9.0
MESH = pl.DeviceIdType.MESH
F32 = jnp.float32


def tau(level):
    return (1.0 / 9.0) * 4.0 ** (level - 1)


def low_lanes():
    return lax.broadcasted_iota(jnp.int32, (1, LANES), 1) < PAIRS


def swap(v):
    return pltpu.roll(v, PAIRS, v.ndim - 1)


def smooth(a, t, x, row, n):
    own = a[t, x, pl.ds(row, n), :]
    total = a[t, x, pl.ds(row - 1, n), :] + a[t, x, pl.ds(row + 1, n), :]
    total = total + (a[t, x - 1, pl.ds(row, n), :] + a[t, x + 1, pl.ds(row, n), :])
    beyond = jnp.where(low_lanes(), a[t + 1, x, pl.ds(row, n), :], a[t - 1, x, pl.ds(row, n), :])
    total = total + swap(own + beyond)
    return own * CENTRE + total * SIDE


def loop(n, body, unroll_below=3):
    if n < unroll_below:
        for i in range(n):
            body(i)
    else:
        lax.fori_loop(0, n, lambda i, c: (body(i), c)[1], 0)


def restrict_rows(r, t, x, rows):
    s = r[t, x, pl.ds(YO, rows, stride=2), :] + r[t, x, pl.ds(YO + 1, rows, stride=2), :]
    s = s + (r[t, x + 1, pl.ds(YO, rows, stride=2), :] + r[t, x + 1, pl.ds(YO + 1, rows, stride=2), :])
    return s + swap(s)


def coarse_cell(r, tc, xc, rows):
    even = restrict_rows(r, 2 * tc + 1, 2 * xc + 1, rows)
    odd = restrict_rows(r, 2 * tc + 2, 2 * xc + 1, rows)
    return jnp.where(low_lanes(), even, odd) * 0.125


def zero_faces(a, tiles, planes, rows):
    flat = jnp.zeros((rows, LANES), F32)
    line = jnp.zeros((1, LANES), F32)

    def body(t):
        a[t + 1, 0, pl.ds(YO, rows), :] = flat
        a[t + 1, planes + 1, pl.ds(YO, rows), :] = flat
        for x in range(1, planes + 1):
            a[t + 1, x, pl.ds(YO - 1, 1), :] = line
            a[t + 1, x, pl.ds(YO + rows, 1), :] = line

    loop(tiles, body)
    for x in range(1, planes + 1):
        a[0, x, pl.ds(YO, rows), :] = flat
        a[tiles + 1, x, pl.ds(YO, rows), :] = flat


def halves(v):
    high = v.astype(jnp.bfloat16)
    return high, (v - high.astype(F32)).astype(jnp.bfloat16)


def dot_t(a, b):
    (ah, al), (bh, bl) = halves(a), halves(b)

    def dot(u, v):
        return lax.dot_general(u, v, (((0,), (0,)), ((), ())), preferred_element_type=F32)

    return dot(ah, bh) + (dot(ah, bl) + dot(al, bh))


def kernel(
    nums, dens, pot, coul,
    f1, h1, r1, w1, f2, h2, r2, w2, f3, h3, r3, w3,
    f4, h4, r4, q4, k4, c4, f5, h5, r5, q5, k5, c5, f6, a6, b6,
    q3, k3, c3, q2, k2, c2, q1, k1, out,
    acc, acc4, cp, ca, cs, cb, ct, cc,
    send, recv, io,
):
    ngx, ngy, ngz = nums
    gx, gy, gz = (lax.axis_index(a) for a in ("gx", "gy", "gz"))
    me = (gx, gy, gz)
    sizes = (ngx, ngy, ngz)
    names = ("gx", "gy", "gz")
    chip, core = gx // 2, gx % 2
    chips = ngx // 2
    counter = [0]
    sent = []

    def has(offset):
        cond = None
        for pos, size, d in zip(me, sizes, offset):
            if d == 0:
                continue
            this = pos + d >= 0 if d < 0 else pos + d < size
            cond = this if cond is None else cond & this
        return cond

    def when(cond, fn):
        if cond is None:
            fn()
        else:
            pl.when(cond)(fn)

    def opposite(offset):
        return tuple(-d for d in offset)

    def near(offset):
        return {n: p + d for n, p, d in zip(names, me, offset) if d != 0}

    class Msg:
        def __init__(self, src, dst, device, cond_send, cond_recv):
            i = counter[0]
            counter[0] += 1
            self.copy = pltpu.make_async_remote_copy(
                src_ref=src, dst_ref=dst, send_sem=send.at[i], recv_sem=recv.at[i], device_id=device, device_id_type=MESH
            )
            self.cond_send, self.cond_recv = cond_send, cond_recv

        def start(self):
            when(self.cond_send, self.copy.start)
            sent.append(self)

        def wait(self):
            when(self.cond_recv, self.copy.wait_recv)

        def drain(self):
            when(self.cond_send, self.copy.wait_send)

    def start(msgs):
        for m in msgs:
            m.start()
        return msgs

    def wait(msgs):
        for m in msgs:
            m.wait()

    offsets = [
        (dx, dy, dz) for dx in (-1, 0, 1) for dy in (-1, 0, 1) for dz in (-1, 0, 1) if (dx, dy, dz) != (0, 0, 0)
    ]
    offsets.sort(key=lambda o: -sum(abs(d) for d in o))

    def order(o):
        return sum(abs(d) for d in o)

    def rim(own, first, widths):
        regions = []
        for o in offsets:
            if order(o) not in widths:
                continue
            src, dst = [], []
            for axis, size, start_at, width in zip((2, 0, 1), own, first, (1, widths[order(o)], widths[order(o)])):
                d = o[axis]
                if d == 0:
                    src.append(pl.ds(start_at, size))
                    dst.append(pl.ds(start_at, size))
                elif d < 0:
                    src.append(pl.ds(start_at, width))
                    dst.append(pl.ds(start_at + size, width))
                else:
                    src.append(pl.ds(start_at + size - width, width))
                    dst.append(pl.ds(start_at - width, width))
            regions.append((o, tuple(src), tuple(dst)))
        return regions

    def exchange(a, own, first, widths):
        return start(
            [
                Msg(a.at[src], a.at[dst], near(o), has(o), has(opposite(o)))
                for o, src, dst in rim(own, first, widths)
            ]
        )

    def clear_outside(a, own, first, widths):
        for o, _, dst in rim(own, first, widths):

            @pl.when(jnp.logical_not(has(opposite(o))))
            def _(dst=dst):
                a[dst + (slice(None),)] = jnp.zeros(tuple(d.size for d in dst) + (LANES,), F32)

    own_1, own_2, own_3 = (8, 16, 16), (4, 8, 8), (2, 4, 4)
    wide = dict(first=(2, 2, YO), widths={1: 2, 2: 1})
    thin = dict(first=(1, 1, YO), widths={1: 1})

    loads = [
        pltpu.make_async_copy(
            dens.at[:, :, pl.ds(t * LANES, LANES)], f1.at[t + 2, pl.ds(2, 16), pl.ds(YO, 16)], io.at[t]
        )
        for t in range(8)
    ]
    for c in loads:
        c.start()
    w2[...] = jnp.zeros(w2.shape, F32)
    w3[...] = jnp.zeros(w3.shape, F32)
    barrier = pltpu.get_barrier_semaphore()
    expected = jnp.int32(0)
    for o in offsets:
        cond = has(o)

        @pl.when(cond)
        def _(o=o):
            pl.semaphore_signal(barrier, inc=1, device_id=near(o), device_id_type=MESH)

        expected = expected + cond.astype(jnp.int32)
    for d in range(1, ngz):
        pl.semaphore_signal(barrier, inc=1, device_id={"gz": lax.rem(gz + d, ngz)}, device_id_type=MESH)
    others = [(dx, dy) for dx in range(ngx) for dy in range(ngy) if (dx, dy) != (0, 0)]

    def other(dx, dy):
        return {"gx": lax.rem(gx + dx, ngx), "gy": lax.rem(gy + dy, ngy)}

    for dx, dy in others:
        pl.semaphore_signal(barrier, inc=1, device_id=other(dx, dy), device_id_type=MESH)
    expected = expected + (ngz - 1 + len(others))

    clear_outside(f1, own_1, **wide)
    for c in loads:
        c.wait()
    pl.semaphore_wait(barrier, expected)
    m_f1 = exchange(f1, own_1, **wide)

    x4, y4, t4 = 2 * ngx, 2 * ngy, ngz
    x5, y5, t5 = x4 // 2, y4 // 2, t4 // 2
    x6, y6, t6 = x5 // 2, y5 // 2, t5 // 2
    clear_outside(r1, own_1, **thin)
    clear_outside(f2, own_2, **wide)
    clear_outside(r2, own_2, **thin)
    clear_outside(f3, own_3, **wide)
    clear_outside(r3, own_3, **thin)
    for a in (f4, h4, r4, q4, k4):
        zero_faces(a, t4, x4, y4)
    c4[...] = jnp.zeros(c4.shape, F32)
    for a in (f5, h5, r5, q5, k5):
        zero_faces(a, t5, x5, y5)
    for a in (f6, a6, b6):
        zero_faces(a, t6, x6, y6)
    acc[...] = jnp.zeros(acc.shape, F32)
    acc4[...] = jnp.zeros(acc4.shape, F32)

    inside = [tuple(c.astype(F32) for c in (p > 0, p < n - 1)) for p, n in zip(me, sizes)]

    def row_mask(n, first, own):
        row = lax.broadcasted_iota(jnp.int32, (n, LANES), 0)
        one = jnp.ones((n, LANES), F32)
        return jnp.where(row < first, one * inside[1][0], jnp.where(row >= first + own, one * inside[1][1], one))

    def side(axis, i, own):
        return inside[axis][0] if i < 0 else inside[axis][1] if i >= own else None

    def masked(v, mask, *scalars):
        v = v * mask
        for s in scalars:
            if s is not None:
                v = v * s
        return v

    def first_step(h, f, own):
        tiles, planes, rows = own
        mask = row_mask(rows + 2, 1, rows)

        def own_tile(t):
            for x in range(-1, planes + 1):
                v = smooth(f, t + 2, x + 2, YO - 1, rows + 2)
                h[t + 1, x + 1, pl.ds(YO - 1, rows + 2), :] = masked(v, mask, side(0, x, planes))

        loop(tiles, own_tile)
        for t in (-1, tiles):
            for x in range(planes):
                h[t + 1, x + 1, pl.ds(YO, rows), :] = smooth(f, t + 2, x + 2, YO, rows) * side(2, t, tiles)

    def apply(dst, src, tiles, planes, rows):
        def body(t):
            for x in range(1, planes + 1):
                dst[t + 1, x, pl.ds(YO, rows), :] = smooth(src, t + 1, x, YO, rows)

        loop(tiles, body)

    def restrict(dst, r, tiles, planes, rows, first=1):
        def body(tc):
            for xc in range(planes):
                dst[tc + first, xc + first, pl.ds(YO, rows), :] = coarse_cell(r, tc, xc, rows)

        loop(tiles, body)

    def collect(w, f, h, r, own, x0, y0, level):
        tiles, planes, rows = own

        def body(t):
            for x in range(planes):
                at = (t + 1, x + 1, pl.ds(YO, rows), slice(None))
                v = f[t + 2, x + 2, pl.ds(YO, rows), :] + h[at] + r[at] + smooth(r, t + 1, x + 1, YO, rows)
                w[t + (x0 > 0), x + x0, pl.ds(y0, rows), :] = v * tau(level)

        loop(tiles, body)

    def energy(f, h, r, own, level):
        tiles, planes, rows = own
        padded = -(-rows // 8) * 8
        keep = lax.broadcasted_iota(jnp.int32, (1, padded, 1), 1) < rows

        def body(t):
            vf = f[t + 2, pl.ds(2, planes), pl.ds(YO, padded), :]
            at = (t + 1, pl.ds(1, planes), pl.ds(YO, padded), slice(None))
            vh, vr = h[at], r[at]
            if padded != rows:
                vf, vh, vr = (jnp.where(keep, v, 0.0) for v in (vf, vh, vr))
            vf, vh, vr = (v.reshape(planes * padded, LANES) for v in (vf, vh, vr))
            acc[...] += (dot_t(vf, vf + vh) + dot_t(vh, vh + vr)) * (tau(level) * 8.0 ** (level - 1))

        loop(tiles, body)

    wait(m_f1)
    first_step(h1, f1, own_1)
    apply(r1, h1, 8, 16, 16)
    restrict(f2, r1, 4, 8, 8, 2)
    m_f2 = exchange(f2, own_2, **wide)
    m_r1 = exchange(r1, own_1, **thin)
    energy(f1, h1, r1, own_1, 1)
    wait(m_f2)
    first_step(h2, f2, own_2)
    apply(r2, h2, 4, 8, 8)
    restrict(f3, r2, 2, 4, 4, 2)
    m_f3 = exchange(f3, own_3, **wide)
    m_r2 = exchange(r2, own_2, **thin)
    energy(f2, h2, r2, own_2, 2)
    wait(m_f3)
    first_step(h3, f3, own_3)
    apply(r3, h3, 2, 4, 4)

    own_x, own_y = pl.ds(2 * gx + 1, 2), pl.ds(YO + 2 * gy, 2)
    for x in range(2):
        f4[gz + 1, 2 * gx + 1 + x, own_y, :] = coarse_cell(r3, 0, x, 2)
    all_t = pl.ds(1, t4)
    block = f4.at[pl.ds(gz + 1, 1), own_x, own_y]
    m_z = start(
        [Msg(block, block, {"gz": lax.rem(gz + d, ngz)}, None, None) for d in range(1, ngz)]
    )
    m_r3 = exchange(r3, own_3, **thin)
    wait(m_r2)
    collect(w2, f2, h2, r2, own_2, 1, 1, 2)
    m_w2 = exchange(w2, own_2, first=(1, 1, 1), widths={1: 1, 2: 1})
    wait(m_r3)
    collect(w3, f3, h3, r3, own_3, 2, 2, 3)
    m_w3 = exchange(w3, own_3, first=(1, 2, 2), widths={1: 2, 2: 2, 3: 2})
    energy(f3, h3, r3, own_3, 3)
    piece = 32 // ngz
    square = acc[0:PAIRS, :] + swap(acc[PAIRS:, :])
    packed = jnp.where(low_lanes(), square[0:32, :], swap(square[32:64, :]))
    for k in range(ngz):
        cp[k] = packed[k * piece : (k + 1) * piece, :]
    m_ca = []
    for d in range(1, ngz):
        to = lax.rem(gz + d, ngz)
        m_ca.append(Msg(cp.at[to], ca.at[gz], {"gz": to}, None, None))
    start(m_ca)
    ca[gz] = cp[gz]

    wait(m_z)
    line = f4.at[all_t, own_x, own_y]
    m_p = []
    for dx in range(chips):
        for dy in range(ngy):
            if (dx, dy) != (0, 0):
                to = {"gx": lax.rem(chip + dx, chips) * 2 + core, "gy": lax.rem(gy + dy, ngy)}
                m_p.append(Msg(line, line, to, None, None))
    start(m_p)
    wait(m_r1)
    collect(w1, f1, h1, r1, own_1, 0, 0, 1)
    wait(m_ca)
    total = ca[0]
    for k in range(1, ngz):
        total = total + ca[k]
    cs[...] = total
    slot = gx * ngy + gy
    cb[slot] = total
    m_cb = start([Msg(cs, cb.at[slot], other(dx, dy), None, None) for dx, dy in others])
    wait(m_p)
    m_c = []
    for j in range(chips):
        part = f4.at[all_t, pl.ds(2 * (2 * j + core) + 1, 2), pl.ds(YO, y4)]
        m_c.append(Msg(part, part, {"gx": 2 * chip + 1 - core}, None, None))
    start(m_c)
    wait(m_c)

    apply(h4, f4, t4, x4, y4)
    apply(r4, h4, t4, x4, y4)
    restrict(f5, r4, t5, x5, y5)
    apply(h5, f5, t5, x5, y5)
    apply(r5, h5, t5, x5, y5)
    restrict(f6, r5, t6, x6, y6)
    for t in range(1, t6 + 1):
        for x in range(1, x6 + 1):
            at = (t, x, pl.ds(YO, y6), slice(None))
            v = f6[at] * tau(6)
            f6[at] = v
            a6[at] = v
    now, later = a6, b6
    for _ in range(7):
        for t in range(1, t6 + 1):
            for x in range(1, x6 + 1):
                at = (t, x, pl.ds(YO, y6), slice(None))
                later[at] = f6[at] + smooth(now, t, x, YO, y6)
        now, later = later, now

    def prolong(dst, value, tile, x, row, rows, which=(0, 1)):
        turned = swap(value)
        halves = (jnp.where(low_lanes(), value, turned), jnp.where(low_lanes(), turned, value))
        for k in which:
            for i in range(2):
                for j in range(2):
                    dst[tile + k, x + i, pl.ds(row + j, rows, stride=2), :] = halves[k]

    def coarse_up(c, f, h, r, q, k, coarse, first, tiles, planes, rows, level, pad):
        def spread(t):
            for x in range(planes // 2):
                value = coarse[t + 1, x + first, pl.ds(YO, rows // 2), :]
                prolong(q, value, 2 * t + 1, 2 * x + 1, YO, rows // 2)

        loop(tiles // 2, spread)
        apply(k, q, tiles, planes, rows)

        def body(t):
            for x in range(1, planes + 1):
                at = (t + 1, x, pl.ds(YO, rows), slice(None))
                v = (f[at] + h[at] + r[at] + smooth(r, t + 1, x, YO, rows)) * tau(level)
                c[t + 1, x + pad, pl.ds(YO, rows), :] = v + smooth(k, t + 1, x, YO, rows)

        loop(tiles, body)

    coarse_up(c5, f5, h5, r5, q5, k5, now, 1, t5, x5, y5, 5, 0)
    coarse_up(c4, f4, h4, r4, q4, k4, c5, 1, t4, x4, y4, 4, 1)

    wait(m_cb)
    total = cb[0]
    for k in range(1, ngx * ngy):
        total = total + cb[k]
    ct[...] = total
    cc[gz] = total
    m_cc = start(
        [Msg(ct, cc.at[gz], {"gz": lax.rem(gz + d, ngz)}, None, None) for d in range(1, ngz)]
    )

    wait(m_w3)
    for j in range(3):
        for i in range(6):
            value = c4[gz + j, 2 * gx + i, pl.ds(YO - 2 + 2 * gy, 6), :]
            prolong(q3, value, 1 + 2 * j, 2 * i, 0, 6)
    mask = row_mask(10, 3, 4)
    for t in range(-2, 4):
        for x in range(-3, 7):
            v = smooth(q3, t + 3, x + 4, 1, 10)
            k3[t + 3, x + 4, pl.ds(1, 10), :] = masked(v, mask, side(2, t, 2), side(0, x, 4))
    mask = row_mask(8, 2, 4)
    for t in range(-1, 3):
        for x in range(-2, 6):
            v = w3[t + 1, x + 2, pl.ds(0, 8), :] + smooth(k3, t + 3, x + 4, 2, 8)
            prolong(q2, masked(v, mask, side(2, t, 2), side(0, x, 4)), 2 * t + 3, 2 * x + 4, 0, 8)

    wait(m_w2)
    mask = row_mask(12, 2, 8)
    for t in range(-1, 5):
        for x in range(-2, 10):
            v = smooth(q2, t + 3, x + 4, 2, 12)
            k2[t + 3, x + 4, pl.ds(2, 12), :] = masked(v, mask, side(2, t, 4), side(0, x, 8))
    mask = row_mask(10, 1, 8)
    for t in range(-1, 5):
        for x in range(-1, 9):
            v = w2[t + 1, x + 1, pl.ds(0, 10), :] + smooth(k2, t + 3, x + 4, 3, 10)
            which = (1,) if t < 0 else (0,) if t >= 4 else (0, 1)
            prolong(q1, masked(v, mask, side(2, t, 4), side(0, x, 8)), 2 * t + 2, 2 * x + 2, 0, 10, which)

    mask = row_mask(18, 1, 16)

    def rim_tile(t):
        for x in range(0, 16):
            v = smooth(q1, t + 2, x + 2, 1, 18)
            k1[t + 2, x + 2, pl.ds(1, 18), :] = masked(v, mask, side(2, t, 8))

    def own_tile(t):
        for x in range(-1, 17):
            v = smooth(q1, t + 2, x + 2, 1, 18)
            k1[t + 2, x + 2, pl.ds(1, 18), :] = masked(v, mask, side(0, x, 16))

    rim_tile(-1)
    rim_tile(8)
    loop(8, own_tile)

    def last(t):
        for x in range(16):
            out[t, x] = w1[t, x] + smooth(k1, t + 2, x + 2, 2, 16)

    loop(8, last)
    stores = [
        pltpu.make_async_copy(out.at[t], pot.at[:, :, pl.ds(t * LANES, LANES)], io.at[t]) for t in range(8)
    ]
    for c in stores:
        c.start()

    padded = -(-y4 // 8) * 8
    keep = lax.broadcasted_iota(jnp.int32, (1, padded, 1), 1) < y4

    def level_4(t):
        vf = f4[t + 1, pl.ds(1, x4), pl.ds(YO, padded), :]
        vc = c4[t + 1, pl.ds(2, x4), pl.ds(YO, padded), :]
        if padded != y4:
            vf, vc = (jnp.where(keep, v, 0.0) for v in (vf, vc))
        acc4[...] += dot_t(vf.reshape(x4 * padded, LANES), vc.reshape(x4 * padded, LANES))

    loop(t4, level_4)
    coarse_part = (acc4[0:PAIRS, :] + swap(acc4[PAIRS:, :])) * 512.0
    wait(m_cc)
    packed = jnp.concatenate([cc[k] for k in range(ngz)], axis=0)
    scale = 4.0 / (ngx * ngy * ngz * 16 * 16 * 16)
    coul[0:32, :] = ((packed + coarse_part[0:32, :]) * scale)[:, :PAIRS]
    coul[32:64, :] = ((swap(packed) + coarse_part[32:64, :]) * scale)[:, :PAIRS]

    for c in stores:
        c.wait()
    for m in sent:
        m.drain()


def local(nums, density):
    ngx, ngy, ngz = nums
    piece = 32 // ngz

    def field(t, x, y):
        return pltpu.VMEM((t, x, y, LANES), F32)

    def level(t, x, y):
        return field(t + 2, x + 2, YO + -(-(y + 1) // 8) * 8)

    t4, x4, y4 = ngz, 2 * ngx, 2 * ngy
    l1, l2, l3 = level(8, 16, 16), level(4, 8, 8), level(2, 4, 4)
    e1, e2, e3 = field(12, 20, 32), field(8, 12, 24), field(6, 8, 16)
    l4, l5, l6 = (level(t4 // s, x4 // s, y4 // s) for s in (1, 2, 4))
    c4 = field(t4 + 2, x4 + 4, 24)
    scratch = [e1, l1, l1, field(8, 16, 16), e2, l2, l2, field(6, 10, 16), e3, l3, l3, field(4, 8, 8)]
    scratch += [l4, l4, l4, l4, l4, c4, l5, l5, l5, l5, l5, l5, l6, l6, l6]
    scratch += [field(8, 12, 16), field(8, 12, 16), field(1, 1, 8), field(10, 16, 16), field(10, 16, 16), field(1, 1, 8)]
    scratch += [field(12, 20, 24), field(12, 20, 24), field(8, 16, 16)]
    square = pltpu.VMEM((LANES, LANES), F32)
    row = pltpu.VMEM((piece, LANES), F32)
    scratch += [square, square, pltpu.VMEM((ngz, piece, LANES), F32), pltpu.VMEM((ngz, piece, LANES), F32), row]
    scratch += [pltpu.VMEM((ngx * ngy, piece, LANES), F32), row, pltpu.VMEM((ngz, piece, LANES), F32)]
    messages = 3 * (18 + 6) + 18 + 26 + 3 * (ngz - 1) + (ngx // 2 * ngy - 1) + (ngx * ngy - 1) + ngx // 2
    scratch += [pltpu.SemaphoreType.DMA((messages,)), pltpu.SemaphoreType.DMA((messages,)), pltpu.SemaphoreType.DMA((8,))]
    return pl.pallas_call(
        functools.partial(kernel, nums),
        out_shape=(
            jax.ShapeDtypeStruct(density.shape, F32),
            jax.ShapeDtypeStruct((PAIRS, PAIRS), F32),
        ),
        in_specs=[pl.BlockSpec(memory_space=pl.ANY)],
        out_specs=(pl.BlockSpec(memory_space=pl.ANY), pl.BlockSpec(memory_space=pltpu.VMEM)),
        scratch_shapes=scratch,
        compiler_params=pltpu.CompilerParams(
            collective_id=0, has_side_effects=True, vmem_limit_bytes=60_000_000
        ),
        name="cycle",
    )(density)


def solution(mesh):
    nums = tuple(mesh.shape[a] for a in ("gx", "gy", "gz"))
    placed = P("gx", "gy", "gz")
    return jax.shard_map(
        functools.partial(local, nums), mesh=mesh, in_specs=(placed,), out_specs=(placed, P()), check_vma=False
    )
```

```python
import functools

import jax
import jax.numpy as jnp
from jax import lax
from jax.experimental import pallas as pl
from jax.experimental.pallas import tpu as pltpu
from jax.sharding import PartitionSpec as P

PAIRS = 64
LANES = 128
YO = 8
CENTRE = 1.0 / 3.0
SIDE = 1.0 / 9.0
MESH = pl.DeviceIdType.MESH
F32 = jnp.float32


def tau(level):
    return (1.0 / 9.0) * 4.0 ** (level - 1)


def low_lanes():
    return lax.broadcasted_iota(jnp.int32, (1, LANES), 1) < PAIRS


def swap(v):
    return pltpu.roll(v, PAIRS, v.ndim - 1)


def smooth(a, t, x, row, n):
    own = a[t, x, pl.ds(row, n), :]
    total = a[t, x, pl.ds(row - 1, n), :] + a[t, x, pl.ds(row + 1, n), :]
    total = total + (a[t, x - 1, pl.ds(row, n), :] + a[t, x + 1, pl.ds(row, n), :])
    beyond = jnp.where(low_lanes(), a[t + 1, x, pl.ds(row, n), :], a[t - 1, x, pl.ds(row, n), :])
    total = total + swap(own + beyond)
    return own * CENTRE + total * SIDE


def loop(n, body, unroll_below=3):
    if n < unroll_below:
        for i in range(n):
            body(i)
    else:
        lax.fori_loop(0, n, lambda i, c: (body(i), c)[1], 0)


def restrict_rows(r, t, x, rows):
    s = r[t, x, pl.ds(YO, rows, stride=2), :] + r[t, x, pl.ds(YO + 1, rows, stride=2), :]
    s = s + (r[t, x + 1, pl.ds(YO, rows, stride=2), :] + r[t, x + 1, pl.ds(YO + 1, rows, stride=2), :])
    return s + swap(s)


def coarse_cell(r, tc, xc, rows):
    even = restrict_rows(r, 2 * tc + 1, 2 * xc + 1, rows)
    odd = restrict_rows(r, 2 * tc + 2, 2 * xc + 1, rows)
    return jnp.where(low_lanes(), even, odd) * 0.125


def zero_faces(a, tiles, planes, rows):
    flat = jnp.zeros((rows, LANES), F32)
    line = jnp.zeros((1, LANES), F32)

    def body(t):
        a[t + 1, 0, pl.ds(YO, rows), :] = flat
        a[t + 1, planes + 1, pl.ds(YO, rows), :] = flat
        for x in range(1, planes + 1):
            a[t + 1, x, pl.ds(YO - 1, 1), :] = line
            a[t + 1, x, pl.ds(YO + rows, 1), :] = line

    loop(tiles, body)
    for x in range(1, planes + 1):
        a[0, x, pl.ds(YO, rows), :] = flat
        a[tiles + 1, x, pl.ds(YO, rows), :] = flat


def halves(v):
    high = v.astype(jnp.bfloat16)
    return high, (v - high.astype(F32)).astype(jnp.bfloat16)


def dot_t(a, b):
    (ah, al), (bh, bl) = halves(a), halves(b)

    def dot(u, v):
        return lax.dot_general(u, v, (((0,), (0,)), ((), ())), preferred_element_type=F32)

    both = dot(ah, jnp.concatenate([bh, bl], axis=1))
    return both[:, :LANES] + (both[:, LANES:] + dot(al, bh))


def kernel(
    nums, dens, pot, coul,
    f1, h1, r1, w1, f2, h2, r2, w2, f3, h3, r3, w3,
    f4, h4, r4, q4, k4, c4, f5, h5, r5, q5, k5, c5, f6, a6, b6,
    q3, k3, c3, q2, k2, c2, q1, k1, out,
    acc, acc4, cp, ca, cs, cb, ct, cc,
    send, recv, io,
):
    ngx, ngy, ngz = nums
    gx, gy, gz = (lax.axis_index(a) for a in ("gx", "gy", "gz"))
    me = (gx, gy, gz)
    sizes = (ngx, ngy, ngz)
    names = ("gx", "gy", "gz")
    chip, core = gx // 2, gx % 2
    chips = ngx // 2
    counter = [0]
    sent = []

    def has(offset):
        cond = None
        for pos, size, d in zip(me, sizes, offset):
            if d == 0:
                continue
            this = pos + d >= 0 if d < 0 else pos + d < size
            cond = this if cond is None else cond & this
        return cond

    def when(cond, fn):
        if cond is None:
            fn()
        else:
            pl.when(cond)(fn)

    def opposite(offset):
        return tuple(-d for d in offset)

    def near(offset):
        return {n: p + d for n, p, d in zip(names, me, offset) if d != 0}

    class Msg:
        def __init__(self, src, dst, device, cond_send, cond_recv):
            i = counter[0]
            counter[0] += 1
            self.copy = pltpu.make_async_remote_copy(
                src_ref=src, dst_ref=dst, send_sem=send.at[i], recv_sem=recv.at[i], device_id=device, device_id_type=MESH
            )
            self.cond_send, self.cond_recv = cond_send, cond_recv

        def start(self):
            when(self.cond_send, self.copy.start)
            sent.append(self)

        def wait(self):
            when(self.cond_recv, self.copy.wait_recv)

        def drain(self):
            when(self.cond_send, self.copy.wait_send)

    def start(msgs):
        for m in msgs:
            m.start()
        return msgs

    def wait(msgs):
        for m in msgs:
            m.wait()

    offsets = [
        (dx, dy, dz) for dx in (-1, 0, 1) for dy in (-1, 0, 1) for dz in (-1, 0, 1) if (dx, dy, dz) != (0, 0, 0)
    ]
    offsets.sort(key=lambda o: -sum(abs(d) for d in o))

    def order(o):
        return sum(abs(d) for d in o)

    def rim(own, first, widths):
        regions = []
        for o in offsets:
            if order(o) not in widths:
                continue
            src, dst = [], []
            for axis, size, start_at, width in zip((2, 0, 1), own, first, (1, widths[order(o)], widths[order(o)])):
                d = o[axis]
                if d == 0:
                    src.append(pl.ds(start_at, size))
                    dst.append(pl.ds(start_at, size))
                elif d < 0:
                    src.append(pl.ds(start_at, width))
                    dst.append(pl.ds(start_at + size, width))
                else:
                    src.append(pl.ds(start_at + size - width, width))
                    dst.append(pl.ds(start_at - width, width))
            regions.append((o, tuple(src), tuple(dst)))
        return regions

    def exchange(a, own, first, widths):
        return start(
            [
                Msg(a.at[src], a.at[dst], near(o), has(o), has(opposite(o)))
                for o, src, dst in rim(own, first, widths)
            ]
        )

    def clear_outside(a, own, first, widths):
        for o, _, dst in rim(own, first, widths):

            @pl.when(jnp.logical_not(has(opposite(o))))
            def _(dst=dst):
                a[dst + (slice(None),)] = jnp.zeros(tuple(d.size for d in dst) + (LANES,), F32)

    own_1, own_2, own_3 = (8, 16, 16), (4, 8, 8), (2, 4, 4)
    wide = dict(first=(2, 2, YO), widths={1: 2, 2: 1})
    thin = dict(first=(1, 1, YO), widths={1: 1})

    loads = [
        pltpu.make_async_copy(
            dens.at[:, :, pl.ds(t * LANES, LANES)], f1.at[t + 2, pl.ds(2, 16), pl.ds(YO, 16)], io.at[t]
        )
        for t in range(8)
    ]
    for c in loads:
        c.start()
    w2[...] = jnp.zeros(w2.shape, F32)
    w3[...] = jnp.zeros(w3.shape, F32)
    barrier = pltpu.get_barrier_semaphore()
    expected = jnp.int32(0)
    for o in offsets:
        cond = has(o)

        @pl.when(cond)
        def _(o=o):
            pl.semaphore_signal(barrier, inc=1, device_id=near(o), device_id_type=MESH)

        expected = expected + cond.astype(jnp.int32)
    for d in range(1, ngz):
        pl.semaphore_signal(barrier, inc=1, device_id={"gz": lax.rem(gz + d, ngz)}, device_id_type=MESH)
    others = [(dx, dy) for dx in range(ngx) for dy in range(ngy) if (dx, dy) != (0, 0)]

    def other(dx, dy):
        return {"gx": lax.rem(gx + dx, ngx), "gy": lax.rem(gy + dy, ngy)}

    for dx, dy in others:
        pl.semaphore_signal(barrier, inc=1, device_id=other(dx, dy), device_id_type=MESH)
    expected = expected + (ngz - 1 + len(others))

    clear_outside(f1, own_1, **wide)
    for c in loads:
        c.wait()
    pl.semaphore_wait(barrier, expected)
    m_f1 = exchange(f1, own_1, **wide)

    x4, y4, t4 = 2 * ngx, 2 * ngy, ngz
    x5, y5, t5 = x4 // 2, y4 // 2, t4 // 2
    x6, y6, t6 = x5 // 2, y5 // 2, t5 // 2
    clear_outside(r1, own_1, **thin)
    clear_outside(f2, own_2, **wide)
    clear_outside(r2, own_2, **thin)
    clear_outside(f3, own_3, **wide)
    clear_outside(r3, own_3, **thin)
    for a in (f4, h4, r4, q4, k4):
        zero_faces(a, t4, x4, y4)
    c4[...] = jnp.zeros(c4.shape, F32)
    for a in (f5, h5, r5, q5, k5):
        zero_faces(a, t5, x5, y5)
    for a in (f6, a6, b6):
        zero_faces(a, t6, x6, y6)
    acc[...] = jnp.zeros(acc.shape, F32)
    acc4[...] = jnp.zeros(acc4.shape, F32)

    inside = [tuple(c.astype(F32) for c in (p > 0, p < n - 1)) for p, n in zip(me, sizes)]

    def row_mask(n, first, own):
        row = lax.broadcasted_iota(jnp.int32, (n, LANES), 0)
        one = jnp.ones((n, LANES), F32)
        return jnp.where(row < first, one * inside[1][0], jnp.where(row >= first + own, one * inside[1][1], one))

    def side(axis, i, own):
        return inside[axis][0] if i < 0 else inside[axis][1] if i >= own else None

    def masked(v, mask, *scalars):
        v = v * mask
        for s in scalars:
            if s is not None:
                v = v * s
        return v

    def first_step(h, f, own):
        tiles, planes, rows = own
        mask = row_mask(rows + 2, 1, rows)

        def own_tile(t):
            for x in range(-1, planes + 1):
                v = smooth(f, t + 2, x + 2, YO - 1, rows + 2)
                h[t + 1, x + 1, pl.ds(YO - 1, rows + 2), :] = masked(v, mask, side(0, x, planes))

        loop(tiles, own_tile)
        for t in (-1, tiles):
            for x in range(planes):
                h[t + 1, x + 1, pl.ds(YO, rows), :] = smooth(f, t + 2, x + 2, YO, rows) * side(2, t, tiles)

    def apply(dst, src, tiles, planes, rows):
        def body(t):
            for x in range(1, planes + 1):
                dst[t + 1, x, pl.ds(YO, rows), :] = smooth(src, t + 1, x, YO, rows)

        loop(tiles, body)

    def restrict(dst, r, tiles, planes, rows, first=1):
        def body(tc):
            for xc in range(planes):
                dst[tc + first, xc + first, pl.ds(YO, rows), :] = coarse_cell(r, tc, xc, rows)

        loop(tiles, body)

    def collect(w, f, h, r, own, x0, y0, level):
        tiles, planes, rows = own

        def body(t):
            for x in range(planes):
                at = (t + 1, x + 1, pl.ds(YO, rows), slice(None))
                v = f[t + 2, x + 2, pl.ds(YO, rows), :] + h[at] + r[at] + smooth(r, t + 1, x + 1, YO, rows)
                w[t + (x0 > 0), x + x0, pl.ds(y0, rows), :] = v * tau(level)

        loop(tiles, body)

    def energy(a, b, own, level):
        tiles, planes, rows = own
        padded = -(-rows // 8) * 8
        step = min(tiles, 4)

        def body(i):
            both = []
            for t in range(step):
                v = a(i * step + t, rows), b(i * step + t, rows)
                if padded != rows:
                    none = jnp.zeros((planes, padded - rows, LANES), F32)
                    v = tuple(jnp.concatenate([u, none], axis=1) for u in v)
                both.append([u.reshape(planes * padded, LANES) for u in v])
            va, vb = (jnp.concatenate(u, axis=0) for u in zip(*both))
            acc[...] += dot_t(va, vb) * 8.0 ** (level - 1)

        loop(tiles // step, body)

    def cells(a, own, first):
        return lambda t, n: a[t + first[0], pl.ds(first[1], own[1]), pl.ds(first[2], n), :]

    wait(m_f1)
    first_step(h1, f1, own_1)
    apply(r1, h1, 8, 16, 16)
    restrict(f2, r1, 4, 8, 8, 2)
    m_f2 = exchange(f2, own_2, **wide)
    m_r1 = exchange(r1, own_1, **thin)
    in_f1, in_h1, in_r1 = (cells(a, own_1, (i, i, YO)) for a, i in ((f1, 2), (h1, 1), (r1, 1)))
    energy(in_f1, lambda t, n: (in_f1(t, n) + in_h1(t, n)) * tau(1), own_1, 1)
    wait(m_f2)
    first_step(h2, f2, own_2)
    apply(r2, h2, 4, 8, 8)
    restrict(f3, r2, 2, 4, 4, 2)
    m_f3 = exchange(f3, own_3, **wide)
    m_r2 = exchange(r2, own_2, **thin)
    energy(in_h1, lambda t, n: (in_h1(t, n) + in_r1(t, n)) * tau(1), own_1, 1)
    wait(m_f3)
    first_step(h3, f3, own_3)
    apply(r3, h3, 2, 4, 4)

    own_x, own_y = pl.ds(2 * gx + 1, 2), pl.ds(YO + 2 * gy, 2)
    for x in range(2):
        f4[gz + 1, 2 * gx + 1 + x, own_y, :] = coarse_cell(r3, 0, x, 2)
    all_t = pl.ds(1, t4)
    block = f4.at[pl.ds(gz + 1, 1), own_x, own_y]
    m_z = start(
        [Msg(block, block, {"gz": lax.rem(gz + d, ngz)}, None, None) for d in range(1, ngz)]
    )
    m_r3 = exchange(r3, own_3, **thin)
    wait(m_r2)
    collect(w2, f2, h2, r2, own_2, 1, 1, 2)
    energy(cells(f2, own_2, (2, 2, YO)), cells(w2, own_2, (1, 1, 1)), own_2, 2)
    wait(m_r3)
    collect(w3, f3, h3, r3, own_3, 2, 2, 3)
    energy(cells(f3, own_3, (2, 2, YO)), cells(w3, own_3, (1, 2, 2)), own_3, 3)
    piece = 32 // ngz
    square = acc[0:PAIRS, :] + swap(acc[PAIRS:, :])
    packed = jnp.where(low_lanes(), square[0:32, :], swap(square[32:64, :]))
    for k in range(ngz):
        cp[k] = packed[k * piece : (k + 1) * piece, :]
    m_ca = []
    for d in range(1, ngz):
        to = lax.rem(gz + d, ngz)
        m_ca.append(Msg(cp.at[to], ca.at[gz], {"gz": to}, None, None))
    start(m_ca)
    ca[gz] = cp[gz]

    wait(m_z)
    line = f4.at[all_t, own_x, own_y]
    m_p = []
    for dx in range(chips):
        for dy in range(ngy):
            if (dx, dy) != (0, 0):
                to = {"gx": lax.rem(chip + dx, chips) * 2 + core, "gy": lax.rem(gy + dy, ngy)}
                m_p.append(Msg(line, line, to, None, None))
    start(m_p)
    m_w3 = exchange(w3, own_3, first=(1, 2, 2), widths={1: 2, 2: 2, 3: 2})
    m_w2 = exchange(w2, own_2, first=(1, 1, 1), widths={1: 1, 2: 1})
    wait(m_r1)
    collect(w1, f1, h1, r1, own_1, 0, 0, 1)
    wait(m_ca)
    total = ca[0]
    for k in range(1, ngz):
        total = total + ca[k]
    cs[...] = total
    slot = gx * ngy + gy
    cb[slot] = total
    m_cb = start([Msg(cs, cb.at[slot], other(dx, dy), None, None) for dx, dy in others])
    wait(m_p)
    m_c = []
    for j in range(chips):
        part = f4.at[all_t, pl.ds(2 * (2 * j + core) + 1, 2), pl.ds(YO, y4)]
        m_c.append(Msg(part, part, {"gx": 2 * chip + 1 - core}, None, None))
    start(m_c)
    wait(m_c)

    apply(h4, f4, t4, x4, y4)
    apply(r4, h4, t4, x4, y4)
    restrict(f5, r4, t5, x5, y5)
    apply(h5, f5, t5, x5, y5)
    apply(r5, h5, t5, x5, y5)
    restrict(f6, r5, t6, x6, y6)
    for t in range(1, t6 + 1):
        for x in range(1, x6 + 1):
            at = (t, x, pl.ds(YO, y6), slice(None))
            v = f6[at] * tau(6)
            f6[at] = v
            a6[at] = v
    now, later = a6, b6
    for _ in range(7):
        for t in range(1, t6 + 1):
            for x in range(1, x6 + 1):
                at = (t, x, pl.ds(YO, y6), slice(None))
                later[at] = f6[at] + smooth(now, t, x, YO, y6)
        now, later = later, now

    def prolong(dst, value, tile, x, row, rows, which=(0, 1)):
        turned = swap(value)
        halves = (jnp.where(low_lanes(), value, turned), jnp.where(low_lanes(), turned, value))
        for k in which:
            for i in range(2):
                for j in range(2):
                    dst[tile + k, x + i, pl.ds(row + j, rows, stride=2), :] = halves[k]

    def coarse_up(c, f, h, r, q, k, coarse, first, tiles, planes, rows, level, pad):
        def spread(t):
            for x in range(planes // 2):
                value = coarse[t + 1, x + first, pl.ds(YO, rows // 2), :]
                prolong(q, value, 2 * t + 1, 2 * x + 1, YO, rows // 2)

        loop(tiles // 2, spread)
        apply(k, q, tiles, planes, rows)

        def body(t):
            for x in range(1, planes + 1):
                at = (t + 1, x, pl.ds(YO, rows), slice(None))
                v = (f[at] + h[at] + r[at] + smooth(r, t + 1, x, YO, rows)) * tau(level)
                c[t + 1, x + pad, pl.ds(YO, rows), :] = v + smooth(k, t + 1, x, YO, rows)

        loop(tiles, body)

    coarse_up(c5, f5, h5, r5, q5, k5, now, 1, t5, x5, y5, 5, 0)
    coarse_up(c4, f4, h4, r4, q4, k4, c5, 1, t4, x4, y4, 4, 1)

    wait(m_cb)
    total = cb[0]
    for k in range(1, ngx * ngy):
        total = total + cb[k]
    ct[...] = total
    cc[gz] = total
    m_cc = start(
        [Msg(ct, cc.at[gz], {"gz": lax.rem(gz + d, ngz)}, None, None) for d in range(1, ngz)]
    )

    wait(m_w3)
    for j in range(3):
        for i in range(6):
            value = c4[gz + j, 2 * gx + i, pl.ds(YO - 2 + 2 * gy, 6), :]
            prolong(q3, value, 1 + 2 * j, 2 * i, 0, 6)
    mask = row_mask(10, 3, 4)
    for t in range(-2, 4):
        for x in range(-3, 7):
            v = smooth(q3, t + 3, x + 4, 1, 10)
            k3[t + 3, x + 4, pl.ds(1, 10), :] = masked(v, mask, side(2, t, 2), side(0, x, 4))
    mask = row_mask(8, 2, 4)
    for t in range(-1, 3):
        for x in range(-2, 6):
            v = w3[t + 1, x + 2, pl.ds(0, 8), :] + smooth(k3, t + 3, x + 4, 2, 8)
            prolong(q2, masked(v, mask, side(2, t, 2), side(0, x, 4)), 2 * t + 3, 2 * x + 4, 0, 8)

    wait(m_w2)
    mask = row_mask(12, 2, 8)
    for t in range(-1, 5):
        for x in range(-2, 10):
            v = smooth(q2, t + 3, x + 4, 2, 12)
            k2[t + 3, x + 4, pl.ds(2, 12), :] = masked(v, mask, side(2, t, 4), side(0, x, 8))
    mask = row_mask(10, 1, 8)
    for t in range(-1, 5):
        for x in range(-1, 9):
            v = w2[t + 1, x + 1, pl.ds(0, 10), :] + smooth(k2, t + 3, x + 4, 3, 10)
            which = (1,) if t < 0 else (0,) if t >= 4 else (0, 1)
            prolong(q1, masked(v, mask, side(2, t, 4), side(0, x, 8)), 2 * t + 2, 2 * x + 2, 0, 10, which)

    mask = row_mask(18, 1, 16)

    def rim_tile(t):
        for x in range(0, 16):
            v = smooth(q1, t + 2, x + 2, 1, 18)
            k1[t + 2, x + 2, pl.ds(1, 18), :] = masked(v, mask, side(2, t, 8))

    def own_tile(t):
        for x in range(-1, 17):
            v = smooth(q1, t + 2, x + 2, 1, 18)
            k1[t + 2, x + 2, pl.ds(1, 18), :] = masked(v, mask, side(0, x, 16))

    rim_tile(-1)
    rim_tile(8)
    loop(8, own_tile)

    def last(t):
        for x in range(16):
            v = w1[t, x] + smooth(k1, t + 2, x + 2, 2, 16)
            pot[x, :, pl.ds(pl.multiple_of(t * LANES, LANES), LANES)] = v

    loop(8, last)
    padded = -(-y4 // 8) * 8
    keep = lax.broadcasted_iota(jnp.int32, (1, padded, 1), 1) < y4

    def level_4(i):
        vf, vc = [], []
        for t in range(4 * i, 4 * i + 4):
            f, c = f4[t + 1, pl.ds(1, x4), pl.ds(YO, padded), :], c4[t + 1, pl.ds(2, x4), pl.ds(YO, padded), :]
            if padded != y4:
                f, c = (jnp.where(keep, v, 0.0) for v in (f, c))
            vf.append(f.reshape(x4 * padded, LANES))
            vc.append(c.reshape(x4 * padded, LANES))
        acc4[...] += dot_t(jnp.concatenate(vf, axis=0), jnp.concatenate(vc, axis=0))

    loop(t4 // 4, level_4)
    coarse_part = (acc4[0:PAIRS, :] + swap(acc4[PAIRS:, :])) * 512.0
    wait(m_cc)
    packed = jnp.concatenate([cc[k] for k in range(ngz)], axis=0)
    scale = 4.0 / (ngx * ngy * ngz * 16 * 16 * 16)
    coul[0:32, :] = ((packed + coarse_part[0:32, :]) * scale)[:, :PAIRS]
    coul[32:64, :] = ((swap(packed) + coarse_part[32:64, :]) * scale)[:, :PAIRS]

    for m in sent:
        m.drain()


def local(nums, density):
    ngx, ngy, ngz = nums
    piece = 32 // ngz

    def field(t, x, y):
        return pltpu.VMEM((t, x, y, LANES), F32)

    def level(t, x, y):
        return field(t + 2, x + 2, YO + -(-(y + 1) // 8) * 8)

    t4, x4, y4 = ngz, 2 * ngx, 2 * ngy
    l1, l2, l3 = level(8, 16, 16), level(4, 8, 8), level(2, 4, 4)
    e1, e2, e3 = field(12, 20, 32), field(8, 12, 24), field(6, 8, 16)
    l4, l5, l6 = (level(t4 // s, x4 // s, y4 // s) for s in (1, 2, 4))
    c4 = field(t4 + 2, x4 + 4, 24)
    scratch = [e1, l1, l1, field(8, 16, 16), e2, l2, l2, field(6, 10, 16), e3, l3, l3, field(4, 8, 8)]
    scratch += [l4, l4, l4, l4, l4, c4, l5, l5, l5, l5, l5, l5, l6, l6, l6]
    scratch += [field(8, 12, 16), field(8, 12, 16), field(1, 1, 8), field(10, 16, 16), field(10, 16, 16), field(1, 1, 8)]
    scratch += [field(12, 20, 24), field(12, 20, 24), field(8, 16, 16)]
    square = pltpu.VMEM((LANES, LANES), F32)
    row = pltpu.VMEM((piece, LANES), F32)
    scratch += [square, square, pltpu.VMEM((ngz, piece, LANES), F32), pltpu.VMEM((ngz, piece, LANES), F32), row]
    scratch += [pltpu.VMEM((ngx * ngy, piece, LANES), F32), row, pltpu.VMEM((ngz, piece, LANES), F32)]
    messages = 3 * (18 + 6) + 18 + 26 + 3 * (ngz - 1) + (ngx // 2 * ngy - 1) + (ngx * ngy - 1) + ngx // 2
    scratch += [pltpu.SemaphoreType.DMA((messages,)), pltpu.SemaphoreType.DMA((messages,)), pltpu.SemaphoreType.DMA((8,))]
    return pl.pallas_call(
        functools.partial(kernel, nums),
        out_shape=(pltpu.VMEM(density.shape, F32), pltpu.VMEM((PAIRS, PAIRS), F32)),
        in_specs=[pl.BlockSpec(memory_space=pl.ANY)],
        out_specs=(pl.BlockSpec(memory_space=pltpu.VMEM), pl.BlockSpec(memory_space=pltpu.VMEM)),
        scratch_shapes=scratch,
        compiler_params=pltpu.CompilerParams(
            collective_id=0, has_side_effects=True, vmem_limit_bytes=65_400_000
        ),
        name="cycle",
    )(density)


def solution(mesh):
    nums = tuple(mesh.shape[a] for a in ("gx", "gy", "gz"))
    placed = P("gx", "gy", "gz")
    return jax.shard_map(
        functools.partial(local, nums), mesh=mesh, in_specs=(placed,), out_specs=(placed, P()), check_vma=False
    )
```

```python
import functools

import jax
import jax.numpy as jnp
from jax import lax
from jax.experimental import pallas as pl
from jax.experimental.pallas import tpu as pltpu
from jax.sharding import PartitionSpec as P

PAIRS = 64
LANES = 128
YO = 8
CENTRE = 1.0 / 3.0
SIDE = 1.0 / 9.0
MESH = pl.DeviceIdType.MESH
F32 = jnp.float32


def tau(level):
    return (1.0 / 9.0) * 4.0 ** (level - 1)


def low_lanes():
    return lax.broadcasted_iota(jnp.int32, (1, LANES), 1) < PAIRS


def swap(v):
    return pltpu.roll(v, PAIRS, v.ndim - 1)


def smooth(a, t, x, row, n):
    own = a[t, x, pl.ds(row, n), :]
    total = a[t, x, pl.ds(row - 1, n), :] + a[t, x, pl.ds(row + 1, n), :]
    total = total + (a[t, x - 1, pl.ds(row, n), :] + a[t, x + 1, pl.ds(row, n), :])
    beyond = jnp.where(low_lanes(), a[t + 1, x, pl.ds(row, n), :], a[t - 1, x, pl.ds(row, n), :])
    total = total + swap(own + beyond)
    return own * CENTRE + total * SIDE


def loop(n, body, unroll_below=3, step=1):
    if n < unroll_below or n <= step:
        for i in range(n):
            body(i)
        return
    step = step if n % step == 0 else 1

    def turn(i, carry):
        for j in range(step):
            body(i * step + j)
        return carry

    lax.fori_loop(0, n // step, turn, 0)


def restrict_rows(r, t, x, rows):
    s = r[t, x, pl.ds(YO, rows, stride=2), :] + r[t, x, pl.ds(YO + 1, rows, stride=2), :]
    s = s + (r[t, x + 1, pl.ds(YO, rows, stride=2), :] + r[t, x + 1, pl.ds(YO + 1, rows, stride=2), :])
    return s + swap(s)


def coarse_cell(r, tc, xc, rows):
    even = restrict_rows(r, 2 * tc + 1, 2 * xc + 1, rows)
    odd = restrict_rows(r, 2 * tc + 2, 2 * xc + 1, rows)
    return jnp.where(low_lanes(), even, odd) * 0.125


def zero_faces(a, tiles, planes, rows):
    flat = jnp.zeros((rows, LANES), F32)
    line = jnp.zeros((1, LANES), F32)

    def body(t):
        a[t + 1, 0, pl.ds(YO, rows), :] = flat
        a[t + 1, planes + 1, pl.ds(YO, rows), :] = flat
        for x in range(1, planes + 1):
            a[t + 1, x, pl.ds(YO - 1, 1), :] = line
            a[t + 1, x, pl.ds(YO + rows, 1), :] = line

    loop(tiles, body)
    for x in range(1, planes + 1):
        a[0, x, pl.ds(YO, rows), :] = flat
        a[tiles + 1, x, pl.ds(YO, rows), :] = flat


def halves(v):
    high = v.astype(jnp.bfloat16)
    return high, (v - high.astype(F32)).astype(jnp.bfloat16)


def dot_t(a, b):
    (ah, al), (bh, bl) = halves(a), halves(b)

    def dot(u, v):
        return lax.dot_general(u, v, (((0,), (0,)), ((), ())), preferred_element_type=F32)

    both = dot(ah, jnp.concatenate([bh, bl], axis=1))
    return both[:, :LANES] + (both[:, LANES:] + dot(al, bh))


def kernel(
    nums, dens, pot, coul,
    f1, h1, r1, w1, f2, h2, r2, w2, f3, h3, r3, w3,
    f4, h4, r4, q4, k4, c4, f5, h5, r5, q5, k5, c5, f6, d6, a6, b6,
    q3, k3, c3, q2, k2, c2, q1, k1, out,
    acc, acc4, cp, ca, cs, cb, ct, cc,
    send, recv, io,
):
    ngx, ngy, ngz = nums
    gx, gy, gz = (lax.axis_index(a) for a in ("gx", "gy", "gz"))
    me = (gx, gy, gz)
    sizes = (ngx, ngy, ngz)
    names = ("gx", "gy", "gz")
    chip, core = gx // 2, gx % 2
    chips = ngx // 2
    counter = [0]
    sent = []

    def has(offset):
        cond = None
        for pos, size, d in zip(me, sizes, offset):
            if d == 0:
                continue
            this = pos + d >= 0 if d < 0 else pos + d < size
            cond = this if cond is None else cond & this
        return cond

    def when(cond, fn):
        if cond is None:
            fn()
        else:
            pl.when(cond)(fn)

    def opposite(offset):
        return tuple(-d for d in offset)

    def near(offset):
        return {n: p + d for n, p, d in zip(names, me, offset) if d != 0}

    class Msg:
        def __init__(self, src, dst, device, cond_send, cond_recv):
            i = counter[0]
            counter[0] += 1
            self.copy = pltpu.make_async_remote_copy(
                src_ref=src, dst_ref=dst, send_sem=send.at[i], recv_sem=recv.at[i], device_id=device, device_id_type=MESH
            )
            self.cond_send, self.cond_recv = cond_send, cond_recv

        def start(self):
            when(self.cond_send, self.copy.start)
            sent.append(self)

        def wait(self):
            when(self.cond_recv, self.copy.wait_recv)

        def drain(self):
            when(self.cond_send, self.copy.wait_send)
            sent.remove(self)

    def start(msgs):
        for m in msgs:
            m.start()
        return msgs

    def drain(msgs):
        for m in msgs:
            m.drain()

    def wait(msgs):
        for m in msgs:
            m.wait()

    offsets = [
        (dx, dy, dz) for dx in (-1, 0, 1) for dy in (-1, 0, 1) for dz in (-1, 0, 1) if (dx, dy, dz) != (0, 0, 0)
    ]
    offsets.sort(key=lambda o: -sum(abs(d) for d in o))

    def order(o):
        return sum(abs(d) for d in o)

    def rim(own, first, widths):
        regions = []
        for o in offsets:
            if order(o) not in widths:
                continue
            src, dst = [], []
            for axis, size, start_at, width in zip((2, 0, 1), own, first, (1, widths[order(o)], widths[order(o)])):
                d = o[axis]
                if d == 0:
                    src.append(pl.ds(start_at, size))
                    dst.append(pl.ds(start_at, size))
                elif d < 0:
                    src.append(pl.ds(start_at, width))
                    dst.append(pl.ds(start_at + size, width))
                else:
                    src.append(pl.ds(start_at + size - width, width))
                    dst.append(pl.ds(start_at - width, width))
            regions.append((o, tuple(src), tuple(dst)))
        return regions

    def exchange(a, own, first, widths):
        return start(
            [
                Msg(a.at[src], a.at[dst], near(o), has(o), has(opposite(o)))
                for o, src, dst in rim(own, first, widths)
            ]
        )

    def clear_outside(a, own, first, widths):
        for o, _, dst in rim(own, first, widths):

            @pl.when(jnp.logical_not(has(opposite(o))))
            def _(dst=dst):
                a[dst + (slice(None),)] = jnp.zeros(tuple(d.size for d in dst) + (LANES,), F32)

    own_1, own_2, own_3 = (8, 16, 16), (4, 8, 8), (2, 4, 4)
    wide = dict(first=(2, 2, YO), widths={1: 2, 2: 1})
    thin = dict(first=(1, 1, YO), widths={1: 1})

    loads = [
        pltpu.make_async_copy(
            dens.at[:, :, pl.ds(t * LANES, LANES)], f1.at[t + 2, pl.ds(2, 16), pl.ds(YO, 16)], io.at[t]
        )
        for t in range(8)
    ]
    for c in loads:
        c.start()
    barrier = pltpu.get_barrier_semaphore()
    expected = jnp.int32(0)
    for o in offsets:
        cond = has(o)

        @pl.when(cond)
        def _(o=o):
            pl.semaphore_signal(barrier, inc=1, device_id=near(o), device_id_type=MESH)

        expected = expected + cond.astype(jnp.int32)
    for d in range(1, ngz):
        pl.semaphore_signal(barrier, inc=1, device_id={"gz": lax.rem(gz + d, ngz)}, device_id_type=MESH)
    others = [(dx, dy) for dx in range(ngx) for dy in range(ngy) if (dx, dy) != (0, 0)]

    def other(dx, dy):
        return {"gx": lax.rem(gx + dx, ngx), "gy": lax.rem(gy + dy, ngy)}

    for dx, dy in others:
        pl.semaphore_signal(barrier, inc=1, device_id=other(dx, dy), device_id_type=MESH)
    expected = expected + (ngz - 1 + len(others))

    for c in loads:
        c.wait()
    pl.semaphore_wait(barrier, expected)
    m_f1 = exchange(f1, own_1, **wide)

    x4, y4, t4 = 2 * ngx, 2 * ngy, ngz
    x5, y5, t5 = x4 // 2, y4 // 2, t4 // 2
    x6, y6, t6 = x5 // 2, y5 // 2, t5 // 2
    rim_2 = dict(first=(1, 1, 1), widths={1: 1, 2: 1})
    rim_3 = dict(first=(1, 2, 2), widths={1: 2, 2: 2, 3: 2})
    clear_outside(f1, own_1, **wide)
    clear_outside(r1, own_1, **thin)
    clear_outside(w2, own_2, **rim_2)
    clear_outside(w3, own_3, **rim_3)
    clear_outside(f2, own_2, **wide)
    clear_outside(r2, own_2, **thin)
    clear_outside(f3, own_3, **wide)
    clear_outside(r3, own_3, **thin)
    for a in (f4, h4, r4, q4, k4):
        zero_faces(a, t4, x4, y4)
    c4[...] = jnp.zeros(c4.shape, F32)
    for a in (f5, h5, r5, q5, k5):
        zero_faces(a, t5, x5, y5)
    for a in (a6, b6):
        zero_faces(a, 2 * t6, x6, y6)
    acc[...] = jnp.zeros(acc.shape, F32)
    acc4[...] = jnp.zeros(acc4.shape, F32)

    inside = [tuple(c.astype(F32) for c in (p > 0, p < n - 1)) for p, n in zip(me, sizes)]

    def row_mask(n, first, own):
        row = lax.broadcasted_iota(jnp.int32, (n, LANES), 0)
        one = jnp.ones((n, LANES), F32)
        return jnp.where(row < first, one * inside[1][0], jnp.where(row >= first + own, one * inside[1][1], one))

    def tile_side(t, own):
        return jnp.where(t < 0, inside[2][0], jnp.where(t >= own, inside[2][1], 1.0))

    def side(axis, i, own):
        return inside[axis][0] if i < 0 else inside[axis][1] if i >= own else None

    def masked(v, mask, *scalars):
        v = v * mask
        for s in scalars:
            if s is not None:
                v = v * s
        return v

    def first_step(h, f, own):
        tiles, planes, rows = own
        mask = row_mask(rows + 2, 1, rows)

        def own_tile(t):
            for x in range(-1, planes + 1):
                v = smooth(f, t + 2, x + 2, YO - 1, rows + 2)
                h[t + 1, x + 1, pl.ds(YO - 1, rows + 2), :] = masked(v, mask, side(0, x, planes))

        loop(tiles, own_tile, step=2 if planes <= 8 else 1)
        for t in (-1, tiles):
            for x in range(planes):
                h[t + 1, x + 1, pl.ds(YO, rows), :] = smooth(f, t + 2, x + 2, YO, rows) * side(2, t, tiles)

    def apply(dst, src, tiles, planes, rows):
        def body(t):
            for x in range(1, planes + 1):
                dst[t + 1, x, pl.ds(YO, rows), :] = smooth(src, t + 1, x, YO, rows)

        loop(tiles, body, step=4 if planes <= 8 else 2 if rows <= 8 else 1)

    def restrict(dst, r, tiles, planes, rows, first=1):
        def body(tc):
            for xc in range(planes):
                dst[tc + first, xc + first, pl.ds(YO, rows), :] = coarse_cell(r, tc, xc, rows)

        loop(tiles, body, step=2)

    def collect(w, f, h, r, own, x0, y0, level):
        tiles, planes, rows = own

        def body(t):
            for x in range(planes):
                at = (t + 1, x + 1, pl.ds(YO, rows), slice(None))
                v = f[t + 2, x + 2, pl.ds(YO, rows), :] + h[at] + r[at] + smooth(r, t + 1, x + 1, YO, rows)
                w[t + (x0 > 0), x + x0, pl.ds(y0, rows), :] = v * tau(level)

        loop(tiles, body)

    def energy(a, b, own, level, total=acc):
        tiles, planes, rows = own
        padded = -(-rows // 8) * 8
        step = min(tiles, 4)

        def body(i):
            both = []
            for t in range(step):
                v = a(i * step + t, rows), b(i * step + t, rows)
                if padded != rows:
                    none = jnp.zeros((planes, padded - rows, LANES), F32)
                    v = tuple(jnp.concatenate([u, none], axis=1) for u in v)
                both.append([u.reshape(planes * padded, LANES) for u in v])
            va, vb = (jnp.concatenate(u, axis=0) for u in zip(*both))
            total[...] += dot_t(va, vb) * 8.0 ** (level - 1)

        loop(tiles // step, body, 2)

    def cells(a, own, first):
        return lambda t, n: a[t + first[0], pl.ds(first[1], own[1]), pl.ds(first[2], n), :]

    wait(m_f1)
    first_step(h1, f1, own_1)
    apply(r1, h1, 8, 16, 16)
    restrict(f2, r1, 4, 8, 8, 2)
    m_f2 = exchange(f2, own_2, **wide)
    m_r1 = exchange(r1, own_1, **thin)
    in_f1, in_h1, in_r1 = (cells(a, own_1, (i, i, YO)) for a, i in ((f1, 2), (h1, 1), (r1, 1)))
    energy(in_f1, lambda t, n: (in_f1(t, n) + in_h1(t, n)) * tau(1), own_1, 1)
    wait(m_f2)
    first_step(h2, f2, own_2)
    apply(r2, h2, 4, 8, 8)
    restrict(f3, r2, 2, 4, 4, 2)
    m_f3 = exchange(f3, own_3, **wide)
    m_r2 = exchange(r2, own_2, **thin)
    energy(in_h1, lambda t, n: (in_h1(t, n) + in_r1(t, n)) * tau(1), own_1, 1)
    in_f2, in_h2, in_r2 = (cells(a, own_2, (i, i, YO)) for a, i in ((f2, 2), (h2, 1), (r2, 1)))
    energy(in_f2, lambda t, n: (in_f2(t, n) + in_h2(t, n)) * tau(2), own_2, 2)
    energy(in_h2, lambda t, n: (in_h2(t, n) + in_r2(t, n)) * tau(2), own_2, 2)
    drain(m_f1)
    wait(m_f3)
    first_step(h3, f3, own_3)
    apply(r3, h3, 2, 4, 4)

    own_x, own_y = pl.ds(2 * gx + 1, 2), pl.ds(YO + 2 * gy, 2)
    for x in range(2):
        f4[gz + 1, 2 * gx + 1 + x, own_y, :] = coarse_cell(r3, 0, x, 2)
    all_t = pl.ds(1, t4)
    block = f4.at[pl.ds(gz + 1, 1), own_x, own_y]
    m_z = start(
        [Msg(block, block, {"gz": lax.rem(gz + d, ngz)}, None, None) for d in range(1, ngz)]
    )
    m_r3 = exchange(r3, own_3, **thin)
    in_f3, in_h3, in_r3 = (cells(a, own_3, (i, i, YO)) for a, i in ((f3, 2), (h3, 1), (r3, 1)))
    energy(in_f3, lambda t, n: (in_f3(t, n) + in_h3(t, n)) * tau(3), own_3, 3)
    energy(in_h3, lambda t, n: (in_h3(t, n) + in_r3(t, n)) * tau(3), own_3, 3)
    piece = 32 // ngz
    square = acc[0:PAIRS, :] + swap(acc[PAIRS:, :])
    packed = jnp.where(low_lanes(), square[0:32, :], swap(square[32:64, :]))
    for k in range(ngz):
        cp[k] = packed[k * piece : (k + 1) * piece, :]
    m_ca = []
    for d in range(1, ngz):
        to = lax.rem(gz + d, ngz)
        m_ca.append(Msg(cp.at[to], ca.at[gz], {"gz": to}, None, None))
    start(m_ca)
    ca[gz] = cp[gz]
    wait(m_r2)
    collect(w2, f2, h2, r2, own_2, 1, 1, 2)
    wait(m_r3)
    collect(w3, f3, h3, r3, own_3, 2, 2, 3)

    drain(m_f2)
    wait(m_z)
    line = f4.at[all_t, own_x, own_y]
    m_p = []
    for dx in range(chips):
        for dy in range(ngy):
            if (dx, dy) != (0, 0):
                to = {"gx": lax.rem(chip + dx, chips) * 2 + core, "gy": lax.rem(gy + dy, ngy)}
                m_p.append(Msg(line, line, to, None, None))
    start(m_p)
    m_w3 = exchange(w3, own_3, **rim_3)
    m_w2 = exchange(w2, own_2, **rim_2)
    wait(m_ca)
    total = ca[0]
    for k in range(1, ngz):
        total = total + ca[k]
    cs[...] = total
    slot = gx * ngy + gy
    cb[slot] = total
    m_cb = start([Msg(cs, cb.at[slot], other(dx, dy), None, None) for dx, dy in others])
    wait(m_r1)
    collect(w1, f1, h1, r1, own_1, 0, 0, 1)
    for m in (m_r1, m_f3, m_r2, m_r3, m_z, m_ca):
        drain(m)
    wait(m_p)
    m_c = []
    for j in range(chips):
        part = f4.at[all_t, pl.ds(2 * (2 * j + core) + 1, 2), pl.ds(YO, y4)]
        m_c.append(Msg(part, part, {"gx": 2 * chip + 1 - core}, None, None))
    start(m_c)
    wait(m_c)

    apply(h4, f4, t4, x4, y4)
    wait(m_cb)
    total = cb[0]
    for k in range(1, ngx * ngy):
        total = total + cb[k]
    ct[...] = total
    cc[gz] = total
    m_cc = start(
        [Msg(ct, cc.at[gz], {"gz": lax.rem(gz + d, ngz)}, None, None) for d in range(1, ngz)]
    )

    apply(r4, h4, t4, x4, y4)
    restrict(f5, r4, t5, x5, y5)
    apply(h5, f5, t5, x5, y5)
    apply(r5, h5, t5, x5, y5)
    restrict(f6, r5, t6, x6, y6)
    cells_6 = [(z, x) for z in range(1, 2 * t6 + 1) for x in range(1, x6 + 1)]
    for t in range(t6):
        for x in range(1, x6 + 1):
            v = f6[t + 1, x, pl.ds(YO, y6), :] * tau(6)
            turned = swap(v)
            for k, u in enumerate((jnp.where(low_lanes(), v, turned), jnp.where(low_lanes(), turned, v))):
                d6[2 * t + 1 + k, x, pl.ds(YO, y6), :] = u
                a6[2 * t + 1 + k, x, pl.ds(YO, y6), :] = u
    now, later = a6, b6
    for _ in range(7):
        for z, x in cells_6:
            own = pl.ds(YO, y6)
            total = now[z, x, pl.ds(YO - 1, y6), :] + now[z, x, pl.ds(YO + 1, y6), :]
            total = total + (now[z, x - 1, own, :] + now[z, x + 1, own, :])
            total = total + (now[z - 1, x, own, :] + now[z + 1, x, own, :])
            later[z, x, own, :] = d6[z, x, own, :] + (now[z, x, own, :] * CENTRE + total * SIDE)
        now, later = later, now

    def prolong(dst, value, tile, x, row, rows, which=(0, 1)):
        turned = swap(value)
        halves = (jnp.where(low_lanes(), value, turned), jnp.where(low_lanes(), turned, value))
        for k in which:
            for i in range(2):
                for j in range(2):
                    dst[tile + k, x + i, pl.ds(row + j, rows, stride=2), :] = halves[k]

    def spread(q, coarse, tiles, planes, rows):
        def body(t):
            for x in range(planes):
                prolong(q, coarse[t + 1, x + 1, pl.ds(YO, rows), :], 2 * t + 1, 2 * x + 1, YO, rows)

        loop(tiles, body, step=2)

    def solved(f, h, r, k, t, x, rows, level):
        at = (t, x, pl.ds(YO, rows), slice(None))
        return (f[at] + h[at] + r[at] + smooth(r, t, x, YO, rows)) * tau(level) + smooth(k, t, x, YO, rows)

    for z, x in cells_6:
        value = now[z, x, pl.ds(YO, y6), :]
        for i in range(2):
            for j in range(2):
                q5[z, 2 * x - 1 + i, pl.ds(YO + j, y6, stride=2), :] = value
    apply(k5, q5, t5, x5, y5)

    def up_c5(t):
        for x in range(1, x5 + 1):
            c5[t + 1, x, pl.ds(YO, y5), :] = solved(f5, h5, r5, k5, t + 1, x, y5, 5)

    loop(t5, up_c5, step=2)
    spread(q4, c5, t5, x5, y5)

    def up_k4(i):
        t = jnp.clip(gz - 2 + i, 0, t4 - 1) + 1
        for j in range(8):
            x = jnp.clip(2 * gx - 3 + j, 0, x4 - 1) + 1
            k4[t, x, pl.ds(YO, y4), :] = smooth(q4, t, x, YO, y4)

    def up_c4(i):
        t = jnp.clip(gz - 1 + i, 0, t4 - 1) + 1
        for j in range(6):
            x = jnp.clip(2 * gx - 2 + j, 0, x4 - 1) + 1
            c4[t, x + 1, pl.ds(YO, y4), :] = solved(f4, h4, r4, k4, t, x, y4, 4)

    loop(5, up_k4, step=5)
    loop(3, up_c4, step=3)

    wait(m_w3)

    def spread_3(j):
        for i in range(6):
            value = c4[gz + j, 2 * gx + i, pl.ds(YO - 2 + 2 * gy, 6), :]
            prolong(q3, value, 1 + 2 * j, 2 * i, 0, 6)

    loop(3, spread_3)
    mask_k3, mask_c3 = row_mask(10, 3, 4), row_mask(8, 2, 4)

    def up_k3(i):
        mask = mask_k3 * tile_side(i - 2, 2)
        for x in range(-3, 7):
            v = smooth(q3, i + 1, x + 4, 1, 10)
            k3[i + 1, x + 4, pl.ds(1, 10), :] = masked(v, mask, side(0, x, 4))

    loop(6, up_k3, step=2)

    def up_c3(i):
        mask = mask_c3 * tile_side(i - 1, 2)
        for x in range(-2, 6):
            v = w3[i, x + 2, pl.ds(0, 8), :] + smooth(k3, i + 2, x + 4, 2, 8)
            prolong(q2, masked(v, mask, side(0, x, 4)), 2 * i + 1, 2 * x + 4, 0, 8)

    loop(4, up_c3, step=2)

    wait(m_w2)
    mask_k2, mask_c2 = row_mask(12, 2, 8), row_mask(10, 1, 8)

    def up_k2(i):
        mask = mask_k2 * tile_side(i - 1, 4)
        for x in range(-2, 10):
            v = smooth(q2, i + 2, x + 4, 2, 12)
            k2[i + 2, x + 4, pl.ds(2, 12), :] = masked(v, mask, side(0, x, 8))

    loop(6, up_k2, step=2)

    def up_c2(i):
        mask = mask_c2 * tile_side(i - 1, 4)
        for x in range(-1, 9):
            v = w2[i, x + 1, pl.ds(0, 10), :] + smooth(k2, i + 2, x + 4, 3, 10)
            prolong(q1, masked(v, mask, side(0, x, 8)), 2 * i, 2 * x + 2, 0, 10)

    loop(6, up_c2, step=2)

    mask = row_mask(18, 1, 16)

    def own_tile(t):
        for x in range(-1, 17):
            v = smooth(q1, t + 2, x + 2, 1, 18)
            k1[t + 2, x + 2, pl.ds(1, 18), :] = masked(v, mask, side(0, x, 16))

    def rim_tile(i):
        for x in range(16):
            v = smooth(q1, 9 * i + 1, x + 2, 2, 16)
            k1[9 * i + 1, x + 2, pl.ds(2, 16), :] = v * jnp.where(i > 0, inside[2][1], inside[2][0])

    loop(2, rim_tile, 2)
    loop(8, own_tile)

    def last(t):
        for x in range(16):
            v = w1[t, x] + smooth(k1, t + 2, x + 2, 2, 16)
            pot[x, :, pl.ds(pl.multiple_of(t * LANES, LANES), LANES)] = v

    loop(8, last)
    in_f4, in_h4, in_r4 = (cells(a, (t4, x4, y4), (1, 1, YO)) for a in (f4, h4, r4))
    energy(in_f4, lambda t, n: (in_f4(t, n) + in_h4(t, n)) * tau(4), (t4, x4, y4), 4, acc4)
    energy(in_h4, lambda t, n: (in_h4(t, n) + in_r4(t, n)) * tau(4), (t4, x4, y4), 4, acc4)
    in_f5, in_c5 = (cells(a, (t5, x5, y5), (1, 1, YO)) for a in (f5, c5))
    energy(in_f5, in_c5, (t5, x5, y5), 5, acc4)
    coarse_part = acc4[0:PAIRS, :] + swap(acc4[PAIRS:, :])
    wait(m_cc)
    packed = jnp.concatenate([cc[k] for k in range(ngz)], axis=0)
    scale = 4.0 / (ngx * ngy * ngz * 16 * 16 * 16)
    coul[0:32, :] = ((packed + coarse_part[0:32, :]) * scale)[:, :PAIRS]
    coul[32:64, :] = ((swap(packed) + coarse_part[32:64, :]) * scale)[:, :PAIRS]

    drain(tuple(sent))


def local(nums, density):
    ngx, ngy, ngz = nums
    piece = 32 // ngz

    def field(t, x, y):
        return pltpu.VMEM((t, x, y, LANES), F32)

    def level(t, x, y):
        return field(t + 2, x + 2, YO + -(-(y + 1) // 8) * 8)

    t4, x4, y4 = ngz, 2 * ngx, 2 * ngy
    l1, l2, l3 = level(8, 16, 16), level(4, 8, 8), level(2, 4, 4)
    e1, e2, e3 = field(12, 20, 32), field(8, 12, 24), field(6, 8, 16)
    l4, l5, l6 = (level(t4 // s, x4 // s, y4 // s) for s in (1, 2, 4))
    e6 = level(t4 // 2, x4 // 4, y4 // 4)
    c4 = field(t4 + 2, x4 + 4, 24)
    scratch = [e1, l1, l1, field(8, 16, 16), e2, l2, l2, field(6, 10, 16), e3, l3, l3, field(4, 8, 8)]
    scratch += [l4, l4, l4, l4, l4, c4, l5, l5, l5, l5, l5, l5, l6, e6, e6, e6]
    scratch += [field(8, 12, 16), field(8, 12, 16), field(1, 1, 8), field(10, 16, 16), field(10, 16, 16), field(1, 1, 8)]
    scratch += [field(12, 20, 24), field(12, 20, 24), field(8, 16, 16)]
    square = pltpu.VMEM((LANES, LANES), F32)
    row = pltpu.VMEM((piece, LANES), F32)
    scratch += [square, square, pltpu.VMEM((ngz, piece, LANES), F32), pltpu.VMEM((ngz, piece, LANES), F32), row]
    scratch += [pltpu.VMEM((ngx * ngy, piece, LANES), F32), row, pltpu.VMEM((ngz, piece, LANES), F32)]
    messages = 3 * (18 + 6) + 18 + 26 + 3 * (ngz - 1) + (ngx // 2 * ngy - 1) + (ngx * ngy - 1) + ngx // 2
    scratch += [pltpu.SemaphoreType.DMA((messages,)), pltpu.SemaphoreType.DMA((messages,)), pltpu.SemaphoreType.DMA((8,))]
    return pl.pallas_call(
        functools.partial(kernel, nums),
        out_shape=(pltpu.VMEM(density.shape, F32), pltpu.VMEM((PAIRS, PAIRS), F32)),
        in_specs=[pl.BlockSpec(memory_space=pl.ANY)],
        out_specs=(pl.BlockSpec(memory_space=pltpu.VMEM), pl.BlockSpec(memory_space=pltpu.VMEM)),
        scratch_shapes=scratch,
        compiler_params=pltpu.CompilerParams(
            collective_id=0, has_side_effects=True, vmem_limit_bytes=65_400_000
        ),
        name="cycle",
    )(density)


def solution(mesh):
    nums = tuple(mesh.shape[a] for a in ("gx", "gy", "gz"))
    placed = P("gx", "gy", "gz")
    return jax.shard_map(
        functools.partial(local, nums), mesh=mesh, in_specs=(placed,), out_specs=(placed, P()), check_vma=False
    )
```

```python
import functools

import jax
import jax.numpy as jnp
from jax import lax
from jax.experimental import pallas as pl
from jax.experimental.pallas import tpu as pltpu
from jax.sharding import PartitionSpec as P

PAIRS = 64
LANES = 128
YO = 8
CENTRE = 1.0 / 3.0
SIDE = 1.0 / 9.0
MESH = pl.DeviceIdType.MESH
F32 = jnp.float32


def tau(level):
    return (1.0 / 9.0) * 4.0 ** (level - 1)


def low_lanes():
    return lax.broadcasted_iota(jnp.int32, (1, LANES), 1) < PAIRS


def swap(v):
    return pltpu.roll(v, PAIRS, v.ndim - 1)


def smooth(a, t, x, row, n):
    own = a[t, x, pl.ds(row, n), :]
    total = a[t, x, pl.ds(row - 1, n), :] + a[t, x, pl.ds(row + 1, n), :]
    total = total + (a[t, x - 1, pl.ds(row, n), :] + a[t, x + 1, pl.ds(row, n), :])
    beyond = jnp.where(low_lanes(), a[t + 1, x, pl.ds(row, n), :], a[t - 1, x, pl.ds(row, n), :])
    total = total + swap(own + beyond)
    return own * CENTRE + total * SIDE


def loop(n, body, unroll_below=3, step=1):
    if n < unroll_below or n <= step:
        for i in range(n):
            body(i)
        return
    step = step if n % step == 0 else 1

    def turn(i, carry):
        for j in range(step):
            body(i * step + j)
        return carry

    lax.fori_loop(0, n // step, turn, 0)


def restrict_rows(r, t, x, rows):
    s = r[t, x, pl.ds(YO, rows, stride=2), :] + r[t, x, pl.ds(YO + 1, rows, stride=2), :]
    s = s + (r[t, x + 1, pl.ds(YO, rows, stride=2), :] + r[t, x + 1, pl.ds(YO + 1, rows, stride=2), :])
    return s + swap(s)


def coarse_cell(r, tc, xc, rows):
    even = restrict_rows(r, 2 * tc + 1, 2 * xc + 1, rows)
    odd = restrict_rows(r, 2 * tc + 2, 2 * xc + 1, rows)
    return jnp.where(low_lanes(), even, odd) * 0.125


def zero_faces(a, tiles, planes, rows):
    flat = jnp.zeros((rows, LANES), F32)
    line = jnp.zeros((1, LANES), F32)

    def body(t):
        a[t + 1, 0, pl.ds(YO, rows), :] = flat
        a[t + 1, planes + 1, pl.ds(YO, rows), :] = flat
        for x in range(1, planes + 1):
            a[t + 1, x, pl.ds(YO - 1, 1), :] = line
            a[t + 1, x, pl.ds(YO + rows, 1), :] = line

    loop(tiles, body)
    for x in range(1, planes + 1):
        a[0, x, pl.ds(YO, rows), :] = flat
        a[tiles + 1, x, pl.ds(YO, rows), :] = flat


def halves(v):
    high = v.astype(jnp.bfloat16)
    return high, (v - high.astype(F32)).astype(jnp.bfloat16)


def dot_t(a, b):
    (ah, al), (bh, bl) = halves(a), halves(b)

    def dot(u, v):
        return lax.dot_general(u, v, (((0,), (0,)), ((), ())), preferred_element_type=F32)

    both = dot(ah, jnp.concatenate([bh, bl], axis=1))
    return both[:, :LANES] + (both[:, LANES:] + dot(al, bh))


def kernel(
    nums, dens, pot, coul,
    f1, h1, r1, w1, f2, h2, r2, w2, f3, h3, r3, w3,
    f4, h4, r4, q4, k4, c4, f5, h5, r5, q5, k5, c5, f6, d6, a6, b6,
    q3, k3, c3, q2, k2, c2, q1, k1, out,
    acc, acc4, cp, ca, cs, cb, ct, cc,
    send, recv, io,
):
    ngx, ngy, ngz = nums
    gx, gy, gz = (lax.axis_index(a) for a in ("gx", "gy", "gz"))
    me = (gx, gy, gz)
    sizes = (ngx, ngy, ngz)
    names = ("gx", "gy", "gz")
    chip, core = gx // 2, gx % 2
    chips = ngx // 2
    counter = [0]
    sent = []

    def has(offset):
        cond = None
        for pos, size, d in zip(me, sizes, offset):
            if d == 0:
                continue
            this = pos + d >= 0 if d < 0 else pos + d < size
            cond = this if cond is None else cond & this
        return cond

    def when(cond, fn):
        if cond is None:
            fn()
        else:
            pl.when(cond)(fn)

    def opposite(offset):
        return tuple(-d for d in offset)

    def near(offset):
        return {n: p + d for n, p, d in zip(names, me, offset) if d != 0}

    class Msg:
        def __init__(self, src, dst, device, cond_send, cond_recv):
            i = counter[0]
            counter[0] += 1
            self.copy = pltpu.make_async_remote_copy(
                src_ref=src, dst_ref=dst, send_sem=send.at[i], recv_sem=recv.at[i], device_id=device, device_id_type=MESH
            )
            self.cond_send, self.cond_recv = cond_send, cond_recv

        def start(self):
            when(self.cond_send, self.copy.start)
            sent.append(self)

        def wait(self):
            when(self.cond_recv, self.copy.wait_recv)

        def drain(self):
            when(self.cond_send, self.copy.wait_send)
            sent.remove(self)

    def start(msgs):
        for m in msgs:
            m.start()
        return msgs

    def drain(msgs):
        for m in msgs:
            m.drain()

    def wait(msgs):
        for m in msgs:
            m.wait()

    offsets = [
        (dx, dy, dz) for dx in (-1, 0, 1) for dy in (-1, 0, 1) for dz in (-1, 0, 1) if (dx, dy, dz) != (0, 0, 0)
    ]
    offsets.sort(key=lambda o: -sum(abs(d) for d in o))

    def order(o):
        return sum(abs(d) for d in o)

    def rim(own, first, widths):
        regions = []
        for o in offsets:
            if order(o) not in widths:
                continue
            src, dst = [], []
            for axis, size, start_at, width in zip((2, 0, 1), own, first, (1, widths[order(o)], widths[order(o)])):
                d = o[axis]
                if d == 0:
                    src.append(pl.ds(start_at, size))
                    dst.append(pl.ds(start_at, size))
                elif d < 0:
                    src.append(pl.ds(start_at, width))
                    dst.append(pl.ds(start_at + size, width))
                else:
                    src.append(pl.ds(start_at + size - width, width))
                    dst.append(pl.ds(start_at - width, width))
            regions.append((o, tuple(src), tuple(dst)))
        return regions

    def exchange(a, own, first, widths):
        return start(
            [
                Msg(a.at[src], a.at[dst], near(o), has(o), has(opposite(o)))
                for o, src, dst in rim(own, first, widths)
            ]
        )

    def clear_outside(a, own, first, widths):
        for o, _, dst in rim(own, first, widths):

            @pl.when(jnp.logical_not(has(opposite(o))))
            def _(dst=dst):
                a[dst + (slice(None),)] = jnp.zeros(tuple(d.size for d in dst) + (LANES,), F32)

    own_1, own_2, own_3 = (8, 16, 16), (4, 8, 8), (2, 4, 4)
    wide = dict(first=(2, 2, YO), widths={1: 2, 2: 1})
    thin = dict(first=(1, 1, YO), widths={1: 1})

    loads = [
        pltpu.make_async_copy(
            dens.at[:, :, pl.ds(t * LANES, LANES)], f1.at[t + 2, pl.ds(2, 16), pl.ds(YO, 16)], io.at[t]
        )
        for t in range(8)
    ]
    for c in loads:
        c.start()
    barrier = pltpu.get_barrier_semaphore()
    expected = jnp.int32(0)
    for o in offsets:
        cond = has(o)

        @pl.when(cond)
        def _(o=o):
            pl.semaphore_signal(barrier, inc=1, device_id=near(o), device_id_type=MESH)

        expected = expected + cond.astype(jnp.int32)
    for d in range(1, ngz):
        pl.semaphore_signal(barrier, inc=1, device_id={"gz": lax.rem(gz + d, ngz)}, device_id_type=MESH)
    others = [(dx, dy) for dx in range(ngx) for dy in range(ngy) if (dx, dy) != (0, 0)]

    def other(dx, dy):
        return {"gx": lax.rem(gx + dx, ngx), "gy": lax.rem(gy + dy, ngy)}

    for dx, dy in others:
        pl.semaphore_signal(barrier, inc=1, device_id=other(dx, dy), device_id_type=MESH)
    expected = expected + (ngz - 1 + len(others))

    for c in loads:
        c.wait()
    pl.semaphore_wait(barrier, expected)
    m_f1 = exchange(f1, own_1, **wide)

    x4, y4, t4 = 2 * ngx, 2 * ngy, ngz
    x5, y5, t5 = x4 // 2, y4 // 2, t4 // 2
    x6, y6, t6 = x5 // 2, y5 // 2, t5 // 2
    rim_2 = dict(first=(1, 1, 1), widths={1: 1, 2: 1})
    rim_3 = dict(first=(1, 2, 2), widths={1: 2, 2: 2, 3: 2})
    clear_outside(f1, own_1, **wide)
    clear_outside(r1, own_1, **thin)
    clear_outside(w2, own_2, **rim_2)
    clear_outside(w3, own_3, **rim_3)
    clear_outside(f2, own_2, **wide)
    clear_outside(r2, own_2, **thin)
    clear_outside(f3, own_3, **wide)
    clear_outside(r3, own_3, **thin)
    for a in (f4, h4, r4, q4, k4):
        zero_faces(a, t4, x4, y4)
    c4[...] = jnp.zeros(c4.shape, F32)
    for a in (f5, h5, r5, q5, k5):
        zero_faces(a, t5, x5, y5)
    for a in (a6, b6):
        zero_faces(a, 2 * t6, x6, y6)
    acc[...] = jnp.zeros(acc.shape, F32)
    acc4[...] = jnp.zeros(acc4.shape, F32)

    inside = [tuple(c.astype(F32) for c in (p > 0, p < n - 1)) for p, n in zip(me, sizes)]

    def row_mask(n, first, own):
        row = lax.broadcasted_iota(jnp.int32, (n, LANES), 0)
        one = jnp.ones((n, LANES), F32)
        return jnp.where(row < first, one * inside[1][0], jnp.where(row >= first + own, one * inside[1][1], one))

    def tile_side(t, own):
        return jnp.where(t < 0, inside[2][0], jnp.where(t >= own, inside[2][1], 1.0))

    def side(axis, i, own):
        return inside[axis][0] if i < 0 else inside[axis][1] if i >= own else None

    def masked(v, mask, *scalars):
        v = v * mask
        for s in scalars:
            if s is not None:
                v = v * s
        return v

    def first_step(h, f, own):
        tiles, planes, rows = own
        mask = row_mask(rows + 2, 1, rows)

        def own_tile(t):
            for x in range(-1, planes + 1):
                v = smooth(f, t + 2, x + 2, YO - 1, rows + 2)
                h[t + 1, x + 1, pl.ds(YO - 1, rows + 2), :] = masked(v, mask, side(0, x, planes))

        loop(tiles, own_tile, step=2)
        for t in (-1, tiles):
            for x in range(planes):
                h[t + 1, x + 1, pl.ds(YO, rows), :] = smooth(f, t + 2, x + 2, YO, rows) * side(2, t, tiles)

    def apply(dst, src, tiles, planes, rows):
        def body(t):
            for x in range(1, planes + 1):
                dst[t + 1, x, pl.ds(YO, rows), :] = smooth(src, t + 1, x, YO, rows)

        loop(tiles, body, step=4 if planes <= 8 else 2)

    def restrict(dst, r, tiles, planes, rows, first=1):
        def body(tc):
            for xc in range(planes):
                dst[tc + first, xc + first, pl.ds(YO, rows), :] = coarse_cell(r, tc, xc, rows)

        loop(tiles, body, step=2)

    def collect(w, f, h, r, own, x0, y0, level):
        tiles, planes, rows = own

        def body(t):
            for x in range(planes):
                at = (t + 1, x + 1, pl.ds(YO, rows), slice(None))
                v = f[t + 2, x + 2, pl.ds(YO, rows), :] + h[at] + r[at] + smooth(r, t + 1, x + 1, YO, rows)
                w[t + (x0 > 0), x + x0, pl.ds(y0, rows), :] = v * tau(level)

        loop(tiles, body)

    def energy(a, b, own, level, total=acc):
        tiles, planes, rows = own
        padded = -(-rows // 8) * 8
        step = min(tiles, 4)

        def body(i):
            both = []
            for t in range(step):
                v = a(i * step + t, rows), b(i * step + t, rows)
                if padded != rows:
                    none = jnp.zeros((planes, padded - rows, LANES), F32)
                    v = tuple(jnp.concatenate([u, none], axis=1) for u in v)
                both.append([u.reshape(planes * padded, LANES) for u in v])
            va, vb = (jnp.concatenate(u, axis=0) for u in zip(*both))
            total[...] += dot_t(va, vb) * 8.0 ** (level - 1)

        loop(tiles // step, body, 2)

    def cells(a, own, first):
        return lambda t, n: a[t + first[0], pl.ds(first[1], own[1]), pl.ds(first[2], n), :]

    wait(m_f1)
    first_step(h1, f1, own_1)
    apply(r1, h1, 8, 16, 16)
    restrict(f2, r1, 4, 8, 8, 2)
    m_f2 = exchange(f2, own_2, **wide)
    m_r1 = exchange(r1, own_1, **thin)
    in_f1, in_h1, in_r1 = (cells(a, own_1, (i, i, YO)) for a, i in ((f1, 2), (h1, 1), (r1, 1)))
    energy(in_f1, lambda t, n: (in_f1(t, n) + in_h1(t, n)) * tau(1), own_1, 1)
    wait(m_f2)
    first_step(h2, f2, own_2)
    apply(r2, h2, 4, 8, 8)
    restrict(f3, r2, 2, 4, 4, 2)
    m_f3 = exchange(f3, own_3, **wide)
    m_r2 = exchange(r2, own_2, **thin)
    energy(in_h1, lambda t, n: (in_h1(t, n) + in_r1(t, n)) * tau(1), own_1, 1)
    in_f2, in_h2, in_r2 = (cells(a, own_2, (i, i, YO)) for a, i in ((f2, 2), (h2, 1), (r2, 1)))
    energy(in_f2, lambda t, n: (in_f2(t, n) + in_h2(t, n)) * tau(2), own_2, 2)
    energy(in_h2, lambda t, n: (in_h2(t, n) + in_r2(t, n)) * tau(2), own_2, 2)
    drain(m_f1)
    wait(m_f3)
    first_step(h3, f3, own_3)
    apply(r3, h3, 2, 4, 4)

    own_x, own_y = pl.ds(2 * gx + 1, 2), pl.ds(YO + 2 * gy, 2)
    for x in range(2):
        f4[gz + 1, 2 * gx + 1 + x, own_y, :] = coarse_cell(r3, 0, x, 2)
    all_t = pl.ds(1, t4)
    block = f4.at[pl.ds(gz + 1, 1), own_x, own_y]
    m_z = start(
        [Msg(block, block, {"gz": lax.rem(gz + d, ngz)}, None, None) for d in range(1, ngz)]
    )
    m_r3 = exchange(r3, own_3, **thin)
    in_f3, in_h3, in_r3 = (cells(a, own_3, (i, i, YO)) for a, i in ((f3, 2), (h3, 1), (r3, 1)))
    energy(in_f3, lambda t, n: (in_f3(t, n) + in_h3(t, n)) * tau(3), own_3, 3)
    energy(in_h3, lambda t, n: (in_h3(t, n) + in_r3(t, n)) * tau(3), own_3, 3)
    piece = 32 // ngz
    square = acc[0:PAIRS, :] + swap(acc[PAIRS:, :])
    packed = jnp.where(low_lanes(), square[0:32, :], swap(square[32:64, :]))
    for k in range(ngz):
        cp[k] = packed[k * piece : (k + 1) * piece, :]
    m_ca = []
    for d in range(1, ngz):
        to = lax.rem(gz + d, ngz)
        m_ca.append(Msg(cp.at[to], ca.at[gz], {"gz": to}, None, None))
    start(m_ca)
    ca[gz] = cp[gz]
    wait(m_r2)
    collect(w2, f2, h2, r2, own_2, 1, 1, 2)
    wait(m_r3)
    collect(w3, f3, h3, r3, own_3, 2, 2, 3)

    drain(m_f2)
    wait(m_z)
    line = f4.at[all_t, own_x, own_y]
    m_p = []
    for dx in range(chips):
        for dy in range(ngy):
            if (dx, dy) != (0, 0):
                to = {"gx": lax.rem(chip + dx, chips) * 2 + core, "gy": lax.rem(gy + dy, ngy)}
                m_p.append(Msg(line, line, to, None, None))
    start(m_p)
    m_w3 = exchange(w3, own_3, **rim_3)
    m_w2 = exchange(w2, own_2, **rim_2)
    wait(m_ca)
    total = ca[0]
    for k in range(1, ngz):
        total = total + ca[k]
    cs[...] = total
    slot = gx * ngy + gy
    cb[slot] = total
    m_cb = start([Msg(cs, cb.at[slot], other(dx, dy), None, None) for dx, dy in others])
    wait(m_r1)
    collect(w1, f1, h1, r1, own_1, 0, 0, 1)
    for m in (m_r1, m_f3, m_r2, m_r3, m_z, m_ca):
        drain(m)
    wait(m_p)
    m_c = []
    for j in range(chips):
        part = f4.at[all_t, pl.ds(2 * (2 * j + core) + 1, 2), pl.ds(YO, y4)]
        m_c.append(Msg(part, part, {"gx": 2 * chip + 1 - core}, None, None))
    start(m_c)
    wait(m_c)

    apply(h4, f4, t4, x4, y4)
    wait(m_cb)
    total = cb[0]
    for k in range(1, ngx * ngy):
        total = total + cb[k]
    ct[...] = total
    cc[gz] = total
    m_cc = start(
        [Msg(ct, cc.at[gz], {"gz": lax.rem(gz + d, ngz)}, None, None) for d in range(1, ngz)]
    )

    apply(r4, h4, t4, x4, y4)
    restrict(f5, r4, t5, x5, y5)
    apply(h5, f5, t5, x5, y5)
    apply(r5, h5, t5, x5, y5)
    restrict(f6, r5, t6, x6, y6)
    cells_6 = [(z, x) for z in range(1, 2 * t6 + 1) for x in range(1, x6 + 1)]
    for t in range(t6):
        for x in range(1, x6 + 1):
            v = f6[t + 1, x, pl.ds(YO, y6), :] * tau(6)
            turned = swap(v)
            for k, u in enumerate((jnp.where(low_lanes(), v, turned), jnp.where(low_lanes(), turned, v))):
                d6[2 * t + 1 + k, x, pl.ds(YO, y6), :] = u
                a6[2 * t + 1 + k, x, pl.ds(YO, y6), :] = u
    now, later = a6, b6
    for _ in range(7):
        for z, x in cells_6:
            own = pl.ds(YO, y6)
            total = now[z, x, pl.ds(YO - 1, y6), :] + now[z, x, pl.ds(YO + 1, y6), :]
            total = total + (now[z, x - 1, own, :] + now[z, x + 1, own, :])
            total = total + (now[z - 1, x, own, :] + now[z + 1, x, own, :])
            later[z, x, own, :] = d6[z, x, own, :] + (now[z, x, own, :] * CENTRE + total * SIDE)
        now, later = later, now

    def prolong(dst, value, tile, x, row, rows, which=(0, 1)):
        turned = swap(value)
        halves = (jnp.where(low_lanes(), value, turned), jnp.where(low_lanes(), turned, value))
        for k in which:
            for i in range(2):
                for j in range(2):
                    dst[tile + k, x + i, pl.ds(row + j, rows, stride=2), :] = halves[k]

    def spread(q, coarse, tiles, planes, rows):
        def body(t):
            for x in range(planes):
                prolong(q, coarse[t + 1, x + 1, pl.ds(YO, rows), :], 2 * t + 1, 2 * x + 1, YO, rows)

        loop(tiles, body, step=2)

    def solved(f, h, r, k, t, x, rows, level):
        at = (t, x, pl.ds(YO, rows), slice(None))
        return (f[at] + h[at] + r[at] + smooth(r, t, x, YO, rows)) * tau(level) + smooth(k, t, x, YO, rows)

    for z, x in cells_6:
        value = now[z, x, pl.ds(YO, y6), :]
        for i in range(2):
            for j in range(2):
                q5[z, 2 * x - 1 + i, pl.ds(YO + j, y6, stride=2), :] = value
    apply(k5, q5, t5, x5, y5)

    def up_c5(t):
        for x in range(1, x5 + 1):
            c5[t + 1, x, pl.ds(YO, y5), :] = solved(f5, h5, r5, k5, t + 1, x, y5, 5)

    loop(t5, up_c5, step=4)
    spread(q4, c5, t5, x5, y5)

    def up_k4(i):
        t = jnp.clip(gz - 2 + i, 0, t4 - 1) + 1
        for j in range(8):
            x = jnp.clip(2 * gx - 3 + j, 0, x4 - 1) + 1
            k4[t, x, pl.ds(YO, y4), :] = smooth(q4, t, x, YO, y4)

    def up_c4(i):
        t = jnp.clip(gz - 1 + i, 0, t4 - 1) + 1
        for j in range(6):
            x = jnp.clip(2 * gx - 2 + j, 0, x4 - 1) + 1
            c4[t, x + 1, pl.ds(YO, y4), :] = solved(f4, h4, r4, k4, t, x, y4, 4)

    loop(5, up_k4, step=5)
    loop(3, up_c4, step=3)

    wait(m_w3)

    def spread_3(j):
        for i in range(6):
            value = c4[gz + j, 2 * gx + i, pl.ds(YO - 2 + 2 * gy, 6), :]
            prolong(q3, value, 1 + 2 * j, 2 * i, 0, 6)

    loop(3, spread_3, step=3)
    mask_k3, mask_c3 = row_mask(10, 3, 4), row_mask(8, 2, 4)

    def up_k3(i):
        mask = mask_k3 * tile_side(i - 2, 2)
        for x in range(-3, 7):
            v = smooth(q3, i + 1, x + 4, 1, 10)
            k3[i + 1, x + 4, pl.ds(1, 10), :] = masked(v, mask, side(0, x, 4))

    loop(6, up_k3, step=6)

    def up_c3(i):
        mask = mask_c3 * tile_side(i - 1, 2)
        for x in range(-2, 6):
            v = w3[i, x + 2, pl.ds(0, 8), :] + smooth(k3, i + 2, x + 4, 2, 8)
            prolong(q2, masked(v, mask, side(0, x, 4)), 2 * i + 1, 2 * x + 4, 0, 8)

    loop(4, up_c3, step=4)

    wait(m_w2)
    mask_k2, mask_c2 = row_mask(12, 2, 8), row_mask(10, 1, 8)

    def up_k2(i):
        mask = mask_k2 * tile_side(i - 1, 4)
        for x in range(-2, 10):
            v = smooth(q2, i + 2, x + 4, 2, 12)
            k2[i + 2, x + 4, pl.ds(2, 12), :] = masked(v, mask, side(0, x, 8))

    loop(6, up_k2, step=3)

    def up_c2(i):
        mask = mask_c2 * tile_side(i - 1, 4)
        for x in range(-1, 9):
            v = w2[i, x + 1, pl.ds(0, 10), :] + smooth(k2, i + 2, x + 4, 3, 10)
            prolong(q1, masked(v, mask, side(0, x, 8)), 2 * i, 2 * x + 2, 0, 10)

    loop(6, up_c2, step=3)

    mask = row_mask(18, 1, 16)

    def own_tile(t):
        for x in range(-1, 17):
            v = smooth(q1, t + 2, x + 2, 1, 18)
            k1[t + 2, x + 2, pl.ds(1, 18), :] = masked(v, mask, side(0, x, 16))

    def rim_tile(i):
        for x in range(16):
            v = smooth(q1, 9 * i + 1, x + 2, 2, 16)
            k1[9 * i + 1, x + 2, pl.ds(2, 16), :] = v * jnp.where(i > 0, inside[2][1], inside[2][0])

    loop(2, rim_tile, 2)
    loop(8, own_tile, step=2)

    def last(t):
        for x in range(16):
            v = w1[t, x] + smooth(k1, t + 2, x + 2, 2, 16)
            pot[x, :, pl.ds(pl.multiple_of(t * LANES, LANES), LANES)] = v

    loop(8, last, step=2)
    in_f4, in_h4, in_r4 = (cells(a, (t4, x4, y4), (1, 1, YO)) for a in (f4, h4, r4))
    energy(in_f4, lambda t, n: (in_f4(t, n) + in_h4(t, n)) * tau(4), (t4, x4, y4), 4, acc4)
    energy(in_h4, lambda t, n: (in_h4(t, n) + in_r4(t, n)) * tau(4), (t4, x4, y4), 4, acc4)
    in_f5, in_c5 = (cells(a, (t5, x5, y5), (1, 1, YO)) for a in (f5, c5))
    energy(in_f5, in_c5, (t5, x5, y5), 5, acc4)
    coarse_part = acc4[0:PAIRS, :] + swap(acc4[PAIRS:, :])
    wait(m_cc)
    packed = jnp.concatenate([cc[k] for k in range(ngz)], axis=0)
    scale = 4.0 / (ngx * ngy * ngz * 16 * 16 * 16)
    coul[0:32, :] = ((packed + coarse_part[0:32, :]) * scale)[:, :PAIRS]
    coul[32:64, :] = ((swap(packed) + coarse_part[32:64, :]) * scale)[:, :PAIRS]

    drain(tuple(sent))


def local(nums, density):
    ngx, ngy, ngz = nums
    piece = 32 // ngz

    def field(t, x, y):
        return pltpu.VMEM((t, x, y, LANES), F32)

    def level(t, x, y):
        return field(t + 2, x + 2, YO + -(-(y + 1) // 8) * 8)

    t4, x4, y4 = ngz, 2 * ngx, 2 * ngy
    l1, l2, l3 = level(8, 16, 16), level(4, 8, 8), level(2, 4, 4)
    e1, e2, e3 = field(12, 20, 32), field(8, 12, 24), field(6, 8, 16)
    l4, l5, l6 = (level(t4 // s, x4 // s, y4 // s) for s in (1, 2, 4))
    e6 = level(t4 // 2, x4 // 4, y4 // 4)
    c4 = field(t4 + 2, x4 + 4, 24)
    scratch = [e1, l1, l1, field(8, 16, 16), e2, l2, l2, field(6, 10, 16), e3, l3, l3, field(4, 8, 8)]
    scratch += [l4, l4, l4, l4, l4, c4, l5, l5, l5, l5, l5, l5, l6, e6, e6, e6]
    scratch += [field(8, 12, 16), field(8, 12, 16), field(1, 1, 8), field(10, 16, 16), field(10, 16, 16), field(1, 1, 8)]
    scratch += [field(12, 20, 24), field(12, 20, 24), field(8, 16, 16)]
    square = pltpu.VMEM((LANES, LANES), F32)
    row = pltpu.VMEM((piece, LANES), F32)
    scratch += [square, square, pltpu.VMEM((ngz, piece, LANES), F32), pltpu.VMEM((ngz, piece, LANES), F32), row]
    scratch += [pltpu.VMEM((ngx * ngy, piece, LANES), F32), row, pltpu.VMEM((ngz, piece, LANES), F32)]
    messages = 3 * (18 + 6) + 18 + 26 + 3 * (ngz - 1) + (ngx // 2 * ngy - 1) + (ngx * ngy - 1) + ngx // 2
    scratch += [pltpu.SemaphoreType.DMA((messages,)), pltpu.SemaphoreType.DMA((messages,)), pltpu.SemaphoreType.DMA((8,))]
    return pl.pallas_call(
        functools.partial(kernel, nums),
        out_shape=(pltpu.VMEM(density.shape, F32), pltpu.VMEM((PAIRS, PAIRS), F32)),
        in_specs=[pl.BlockSpec(memory_space=pl.ANY)],
        out_specs=(pl.BlockSpec(memory_space=pltpu.VMEM), pl.BlockSpec(memory_space=pltpu.VMEM)),
        scratch_shapes=scratch,
        compiler_params=pltpu.CompilerParams(
            collective_id=0, has_side_effects=True, vmem_limit_bytes=65_400_000
        ),
        name="cycle",
    )(density)


def solution(mesh):
    nums = tuple(mesh.shape[a] for a in ("gx", "gy", "gz"))
    placed = P("gx", "gy", "gz")
    return jax.shard_map(
        functools.partial(local, nums), mesh=mesh, in_specs=(placed,), out_specs=(placed, P()), check_vma=False
    )
```

```python
import functools

import jax
import jax.numpy as jnp
from jax import lax
from jax.experimental import pallas as pl
from jax.experimental.pallas import tpu as pltpu
from jax.sharding import PartitionSpec as P

PAIRS = 64
LANES = 128
YO = 8
CENTRE = 1.0 / 3.0
SIDE = 1.0 / 9.0
MESH = pl.DeviceIdType.MESH
F32 = jnp.float32


def tau(level):
    return (1.0 / 9.0) * 4.0 ** (level - 1)


def low_lanes():
    return lax.broadcasted_iota(jnp.int32, (1, LANES), 1) < PAIRS


def swap(v):
    return pltpu.roll(v, PAIRS, v.ndim - 1)


def smooth(a, t, x, row, n):
    own = a[t, x, pl.ds(row, n), :]
    total = a[t, x, pl.ds(row - 1, n), :] + a[t, x, pl.ds(row + 1, n), :]
    total = total + (a[t, x - 1, pl.ds(row, n), :] + a[t, x + 1, pl.ds(row, n), :])
    beyond = jnp.where(low_lanes(), a[t + 1, x, pl.ds(row, n), :], a[t - 1, x, pl.ds(row, n), :])
    total = total + swap(own + beyond)
    return own * CENTRE + total * SIDE


def loop(n, body, unroll_below=3, step=1):
    if n < unroll_below or n <= step:
        for i in range(n):
            body(i)
        return
    step = step if n % step == 0 else 1

    def turn(i, carry):
        for j in range(step):
            body(i * step + j)
        return carry

    lax.fori_loop(0, n // step, turn, 0)


def restrict_rows(r, t, x, rows):
    s = r[t, x, pl.ds(YO, rows, stride=2), :] + r[t, x, pl.ds(YO + 1, rows, stride=2), :]
    s = s + (r[t, x + 1, pl.ds(YO, rows, stride=2), :] + r[t, x + 1, pl.ds(YO + 1, rows, stride=2), :])
    return s + swap(s)


def coarse_cell(r, tc, xc, rows):
    even = restrict_rows(r, 2 * tc + 1, 2 * xc + 1, rows)
    odd = restrict_rows(r, 2 * tc + 2, 2 * xc + 1, rows)
    return jnp.where(low_lanes(), even, odd) * 0.125


def zero_faces(a, tiles, planes, rows):
    flat = jnp.zeros((rows, LANES), F32)
    line = jnp.zeros((1, LANES), F32)

    def body(t):
        a[t + 1, 0, pl.ds(YO, rows), :] = flat
        a[t + 1, planes + 1, pl.ds(YO, rows), :] = flat
        for x in range(1, planes + 1):
            a[t + 1, x, pl.ds(YO - 1, 1), :] = line
            a[t + 1, x, pl.ds(YO + rows, 1), :] = line

    loop(tiles, body)
    for x in range(1, planes + 1):
        a[0, x, pl.ds(YO, rows), :] = flat
        a[tiles + 1, x, pl.ds(YO, rows), :] = flat


def halves(v):
    high = v.astype(jnp.bfloat16)
    return high, (v - high.astype(F32)).astype(jnp.bfloat16)


def dot_t(a, b):
    (ah, al), (bh, bl) = halves(a), halves(b)

    def dot(u, v):
        return lax.dot_general(u, v, (((0,), (0,)), ((), ())), preferred_element_type=F32)

    both = dot(ah, jnp.concatenate([bh, bl], axis=1))
    return both[:, :LANES] + (both[:, LANES:] + dot(al, bh))


def kernel(
    nums, dens, pot, coul,
    f1, h1, r1, w1, f2, h2, r2, w2, f3, h3, r3, w3,
    f4, h4, r4, q4, k4, c4, f5, h5, r5, q5, k5, c5, f6, d6, a6, b6,
    q3, k3, c3, q2, k2, c2, q1, k1, out,
    acc, acc4, cp, ca, cs, cb, ct, cc,
    send, recv, io,
):
    ngx, ngy, ngz = nums
    gx, gy, gz = (lax.axis_index(a) for a in ("gx", "gy", "gz"))
    me = (gx, gy, gz)
    sizes = (ngx, ngy, ngz)
    names = ("gx", "gy", "gz")
    chip, core = gx // 2, gx % 2
    chips = ngx // 2
    counter = [0]
    sent = []

    def has(offset):
        cond = None
        for pos, size, d in zip(me, sizes, offset):
            if d == 0:
                continue
            this = pos + d >= 0 if d < 0 else pos + d < size
            cond = this if cond is None else cond & this
        return cond

    def when(cond, fn):
        if cond is None:
            fn()
        else:
            pl.when(cond)(fn)

    def opposite(offset):
        return tuple(-d for d in offset)

    def near(offset):
        return {n: p + d for n, p, d in zip(names, me, offset) if d != 0}

    class Msg:
        def __init__(self, src, dst, device, cond_send, cond_recv):
            i = counter[0]
            counter[0] += 1
            self.copy = pltpu.make_async_remote_copy(
                src_ref=src, dst_ref=dst, send_sem=send.at[i], recv_sem=recv.at[i], device_id=device, device_id_type=MESH
            )
            self.cond_send, self.cond_recv = cond_send, cond_recv

        def start(self):
            when(self.cond_send, self.copy.start)
            sent.append(self)

        def wait(self):
            when(self.cond_recv, self.copy.wait_recv)

        def drain(self):
            when(self.cond_send, self.copy.wait_send)
            sent.remove(self)

    def start(msgs):
        for m in msgs:
            m.start()
        return msgs

    def drain(msgs):
        for m in msgs:
            m.drain()

    def wait(msgs):
        for m in msgs:
            m.wait()

    offsets = [
        (dx, dy, dz) for dx in (-1, 0, 1) for dy in (-1, 0, 1) for dz in (-1, 0, 1) if (dx, dy, dz) != (0, 0, 0)
    ]
    offsets.sort(key=lambda o: -sum(abs(d) for d in o))

    def order(o):
        return sum(abs(d) for d in o)

    def rim(own, first, widths):
        regions = []
        for o in offsets:
            if order(o) not in widths:
                continue
            src, dst = [], []
            for axis, size, start_at, width in zip((2, 0, 1), own, first, (1, widths[order(o)], widths[order(o)])):
                d = o[axis]
                if d == 0:
                    src.append(pl.ds(start_at, size))
                    dst.append(pl.ds(start_at, size))
                elif d < 0:
                    src.append(pl.ds(start_at, width))
                    dst.append(pl.ds(start_at + size, width))
                else:
                    src.append(pl.ds(start_at + size - width, width))
                    dst.append(pl.ds(start_at - width, width))
            regions.append((o, tuple(src), tuple(dst)))
        return regions

    def exchange(a, own, first, widths):
        return start(
            [
                Msg(a.at[src], a.at[dst], near(o), has(o), has(opposite(o)))
                for o, src, dst in rim(own, first, widths)
            ]
        )

    def clear_outside(a, own, first, widths):
        for o, _, dst in rim(own, first, widths):

            @pl.when(jnp.logical_not(has(opposite(o))))
            def _(dst=dst):
                a[dst + (slice(None),)] = jnp.zeros(tuple(d.size for d in dst) + (LANES,), F32)

    own_1, own_2, own_3 = (8, 16, 16), (4, 8, 8), (2, 4, 4)
    wide = dict(first=(2, 2, YO), widths={1: 2, 2: 1})
    thin = dict(first=(1, 1, YO), widths={1: 1})

    loads = [
        pltpu.make_async_copy(
            dens.at[:, :, pl.ds(t * LANES, LANES)], f1.at[t + 2, pl.ds(2, 16), pl.ds(YO, 16)], io.at[t]
        )
        for t in range(8)
    ]
    for c in loads:
        c.start()
    barrier = pltpu.get_barrier_semaphore()
    expected = jnp.int32(0)
    for o in offsets:
        cond = has(o)

        @pl.when(cond)
        def _(o=o):
            pl.semaphore_signal(barrier, inc=1, device_id=near(o), device_id_type=MESH)

        expected = expected + cond.astype(jnp.int32)
    for d in range(1, ngz):
        pl.semaphore_signal(barrier, inc=1, device_id={"gz": lax.rem(gz + d, ngz)}, device_id_type=MESH)
    others = [(dx, dy) for dx in range(ngx) for dy in range(ngy) if (dx, dy) != (0, 0)]

    def other(dx, dy):
        return {"gx": lax.rem(gx + dx, ngx), "gy": lax.rem(gy + dy, ngy)}

    for dx, dy in others:
        pl.semaphore_signal(barrier, inc=1, device_id=other(dx, dy), device_id_type=MESH)
    expected = expected + (ngz - 1 + len(others))

    for c in loads:
        c.wait()
    pl.semaphore_wait(barrier, expected)
    m_f1 = exchange(f1, own_1, **wide)

    x4, y4, t4 = 2 * ngx, 2 * ngy, ngz
    x5, y5, t5 = x4 // 2, y4 // 2, t4 // 2
    x6, y6, t6 = x5 // 2, y5 // 2, t5 // 2
    rim_2 = dict(first=(1, 1, 1), widths={1: 1, 2: 1})
    rim_3 = dict(first=(1, 2, 2), widths={1: 2, 2: 2, 3: 2})
    clear_outside(f1, own_1, **wide)
    clear_outside(r1, own_1, **thin)
    clear_outside(w2, own_2, **rim_2)
    clear_outside(w3, own_3, **rim_3)
    clear_outside(f2, own_2, **wide)
    clear_outside(r2, own_2, **thin)
    clear_outside(f3, own_3, **wide)
    clear_outside(r3, own_3, **thin)
    for a in (f4, h4, r4, q4, k4):
        zero_faces(a, t4, x4, y4)
    c4[...] = jnp.zeros(c4.shape, F32)
    for a in (f5, h5, r5, q5, k5):
        zero_faces(a, t5, x5, y5)
    for a in (a6, b6):
        zero_faces(a, 2 * t6, x6, y6)
    acc[...] = jnp.zeros(acc.shape, F32)
    acc4[...] = jnp.zeros(acc4.shape, F32)

    inside = [tuple(c.astype(F32) for c in (p > 0, p < n - 1)) for p, n in zip(me, sizes)]

    def row_mask(n, first, own):
        row = lax.broadcasted_iota(jnp.int32, (n, LANES), 0)
        one = jnp.ones((n, LANES), F32)
        return jnp.where(row < first, one * inside[1][0], jnp.where(row >= first + own, one * inside[1][1], one))

    def tile_side(t, own):
        return jnp.where(t < 0, inside[2][0], jnp.where(t >= own, inside[2][1], 1.0))

    def side(axis, i, own):
        return inside[axis][0] if i < 0 else inside[axis][1] if i >= own else None

    def masked(v, mask, *scalars):
        v = v * mask
        for s in scalars:
            if s is not None:
                v = v * s
        return v

    def first_step(h, f, own):
        tiles, planes, rows = own
        mask = row_mask(rows + 2, 1, rows)

        def own_tile(t):
            for x in range(-1, planes + 1):
                v = smooth(f, t + 2, x + 2, YO - 1, rows + 2)
                h[t + 1, x + 1, pl.ds(YO - 1, rows + 2), :] = masked(v, mask, side(0, x, planes))

        loop(tiles, own_tile, step=2)
        for t in (-1, tiles):
            for x in range(planes):
                h[t + 1, x + 1, pl.ds(YO, rows), :] = smooth(f, t + 2, x + 2, YO, rows) * side(2, t, tiles)

    def apply(dst, src, tiles, planes, rows):
        def body(t):
            for x in range(1, planes + 1):
                dst[t + 1, x, pl.ds(YO, rows), :] = smooth(src, t + 1, x, YO, rows)

        loop(tiles, body, step=4 if rows <= 8 else 2)

    def restrict(dst, r, tiles, planes, rows, first=1):
        def body(tc):
            for xc in range(planes):
                dst[tc + first, xc + first, pl.ds(YO, rows), :] = coarse_cell(r, tc, xc, rows)

        loop(tiles, body, step=4)

    def collect(w, f, h, r, own, x0, y0, level):
        tiles, planes, rows = own

        def body(t):
            for x in range(planes):
                at = (t + 1, x + 1, pl.ds(YO, rows), slice(None))
                v = f[t + 2, x + 2, pl.ds(YO, rows), :] + h[at] + r[at] + smooth(r, t + 1, x + 1, YO, rows)
                w[t + (x0 > 0), x + x0, pl.ds(y0, rows), :] = v * tau(level)

        loop(tiles, body)

    def energy(a, b, own, level, total=acc):
        tiles, planes, rows = own
        padded = -(-rows // 8) * 8
        step = min(tiles, 4)

        def body(i):
            both = []
            for t in range(step):
                v = a(i * step + t, rows), b(i * step + t, rows)
                if padded != rows:
                    none = jnp.zeros((planes, padded - rows, LANES), F32)
                    v = tuple(jnp.concatenate([u, none], axis=1) for u in v)
                both.append([u.reshape(planes * padded, LANES) for u in v])
            va, vb = (jnp.concatenate(u, axis=0) for u in zip(*both))
            total[...] += dot_t(va, vb) * 8.0 ** (level - 1)

        loop(tiles // step, body, 2)

    def cells(a, own, first):
        return lambda t, n: a[t + first[0], pl.ds(first[1], own[1]), pl.ds(first[2], n), :]

    wait(m_f1)
    first_step(h1, f1, own_1)
    apply(r1, h1, 8, 16, 16)
    restrict(f2, r1, 4, 8, 8, 2)
    m_f2 = exchange(f2, own_2, **wide)
    m_r1 = exchange(r1, own_1, **thin)
    in_f1, in_h1, in_r1 = (cells(a, own_1, (i, i, YO)) for a, i in ((f1, 2), (h1, 1), (r1, 1)))
    energy(in_f1, lambda t, n: (in_f1(t, n) + in_h1(t, n)) * tau(1), own_1, 1)
    wait(m_f2)
    first_step(h2, f2, own_2)
    apply(r2, h2, 4, 8, 8)
    restrict(f3, r2, 2, 4, 4, 2)
    m_f3 = exchange(f3, own_3, **wide)
    m_r2 = exchange(r2, own_2, **thin)
    energy(in_h1, lambda t, n: (in_h1(t, n) + in_r1(t, n)) * tau(1), own_1, 1)
    in_f2, in_h2, in_r2 = (cells(a, own_2, (i, i, YO)) for a, i in ((f2, 2), (h2, 1), (r2, 1)))
    energy(in_f2, lambda t, n: (in_f2(t, n) + in_h2(t, n)) * tau(2), own_2, 2)
    energy(in_h2, lambda t, n: (in_h2(t, n) + in_r2(t, n)) * tau(2), own_2, 2)
    drain(m_f1)
    wait(m_f3)
    first_step(h3, f3, own_3)
    apply(r3, h3, 2, 4, 4)

    own_x, own_y = pl.ds(2 * gx + 1, 2), pl.ds(YO + 2 * gy, 2)
    for x in range(2):
        f4[gz + 1, 2 * gx + 1 + x, own_y, :] = coarse_cell(r3, 0, x, 2)
    all_t = pl.ds(1, t4)
    block = f4.at[pl.ds(gz + 1, 1), own_x, own_y]
    m_z = start(
        [Msg(block, block, {"gz": lax.rem(gz + d, ngz)}, None, None) for d in range(1, ngz)]
    )
    m_r3 = exchange(r3, own_3, **thin)
    in_f3, in_h3, in_r3 = (cells(a, own_3, (i, i, YO)) for a, i in ((f3, 2), (h3, 1), (r3, 1)))
    energy(in_f3, lambda t, n: (in_f3(t, n) + in_h3(t, n)) * tau(3), own_3, 3)
    energy(in_h3, lambda t, n: (in_h3(t, n) + in_r3(t, n)) * tau(3), own_3, 3)
    piece = 32 // ngz
    square = acc[0:PAIRS, :] + swap(acc[PAIRS:, :])
    packed = jnp.where(low_lanes(), square[0:32, :], swap(square[32:64, :]))
    for k in range(ngz):
        cp[k] = packed[k * piece : (k + 1) * piece, :]
    m_ca = []
    for d in range(1, ngz):
        to = lax.rem(gz + d, ngz)
        m_ca.append(Msg(cp.at[to], ca.at[gz], {"gz": to}, None, None))
    start(m_ca)
    ca[gz] = cp[gz]
    wait(m_r2)
    collect(w2, f2, h2, r2, own_2, 1, 1, 2)
    wait(m_r3)
    collect(w3, f3, h3, r3, own_3, 2, 2, 3)

    drain(m_f2)
    wait(m_z)
    line = f4.at[all_t, own_x, own_y]
    m_p = []
    for dx in range(chips):
        for dy in range(ngy):
            if (dx, dy) != (0, 0):
                to = {"gx": lax.rem(chip + dx, chips) * 2 + core, "gy": lax.rem(gy + dy, ngy)}
                m_p.append(Msg(line, line, to, None, None))
    start(m_p)
    m_w3 = exchange(w3, own_3, **rim_3)
    m_w2 = exchange(w2, own_2, **rim_2)
    wait(m_ca)
    total = ca[0]
    for k in range(1, ngz):
        total = total + ca[k]
    cs[...] = total
    slot = gx * ngy + gy
    cb[slot] = total
    m_cb = start([Msg(cs, cb.at[slot], other(dx, dy), None, None) for dx, dy in others])
    wait(m_r1)
    collect(w1, f1, h1, r1, own_1, 0, 0, 1)
    for m in (m_r1, m_f3, m_r2, m_r3, m_z, m_ca):
        drain(m)
    wait(m_p)
    m_c = []
    for j in range(chips):
        part = f4.at[all_t, pl.ds(2 * (2 * j + core) + 1, 2), pl.ds(YO, y4)]
        m_c.append(Msg(part, part, {"gx": 2 * chip + 1 - core}, None, None))
    start(m_c)
    wait(m_c)

    apply(h4, f4, t4, x4, y4)
    wait(m_cb)
    total = cb[0]
    for k in range(1, ngx * ngy):
        total = total + cb[k]
    ct[...] = total
    cc[gz] = total
    m_cc = start(
        [Msg(ct, cc.at[gz], {"gz": lax.rem(gz + d, ngz)}, None, None) for d in range(1, ngz)]
    )

    apply(r4, h4, t4, x4, y4)
    restrict(f5, r4, t5, x5, y5)
    apply(h5, f5, t5, x5, y5)
    apply(r5, h5, t5, x5, y5)
    restrict(f6, r5, t6, x6, y6)
    cells_6 = [(z, x) for z in range(1, 2 * t6 + 1) for x in range(1, x6 + 1)]
    for t in range(t6):
        for x in range(1, x6 + 1):
            v = f6[t + 1, x, pl.ds(YO, y6), :] * tau(6)
            turned = swap(v)
            for k, u in enumerate((jnp.where(low_lanes(), v, turned), jnp.where(low_lanes(), turned, v))):
                d6[2 * t + 1 + k, x, pl.ds(YO, y6), :] = u
                a6[2 * t + 1 + k, x, pl.ds(YO, y6), :] = u
    now, later = a6, b6
    for _ in range(7):
        for z, x in cells_6:
            own = pl.ds(YO, y6)
            total = now[z, x, pl.ds(YO - 1, y6), :] + now[z, x, pl.ds(YO + 1, y6), :]
            total = total + (now[z, x - 1, own, :] + now[z, x + 1, own, :])
            total = total + (now[z - 1, x, own, :] + now[z + 1, x, own, :])
            later[z, x, own, :] = d6[z, x, own, :] + (now[z, x, own, :] * CENTRE + total * SIDE)
        now, later = later, now

    def prolong(dst, value, tile, x, row, rows, which=(0, 1)):
        turned = swap(value)
        halves = (jnp.where(low_lanes(), value, turned), jnp.where(low_lanes(), turned, value))
        for k in which:
            for i in range(2):
                for j in range(2):
                    dst[tile + k, x + i, pl.ds(row + j, rows, stride=2), :] = halves[k]

    def spread(q, coarse, tiles, planes, rows):
        def body(t):
            for x in range(planes):
                prolong(q, coarse[t + 1, x + 1, pl.ds(YO, rows), :], 2 * t + 1, 2 * x + 1, YO, rows)

        loop(tiles, body, step=2)

    def solved(f, h, r, k, t, x, rows, level):
        at = (t, x, pl.ds(YO, rows), slice(None))
        return (f[at] + h[at] + r[at] + smooth(r, t, x, YO, rows)) * tau(level) + smooth(k, t, x, YO, rows)

    for z, x in cells_6:
        value = now[z, x, pl.ds(YO, y6), :]
        for i in range(2):
            for j in range(2):
                q5[z, 2 * x - 1 + i, pl.ds(YO + j, y6, stride=2), :] = value
    apply(k5, q5, t5, x5, y5)

    def up_c5(t):
        for x in range(1, x5 + 1):
            c5[t + 1, x, pl.ds(YO, y5), :] = solved(f5, h5, r5, k5, t + 1, x, y5, 5)

    loop(t5, up_c5, step=4)
    spread(q4, c5, t5, x5, y5)

    def up_k4(i):
        t = jnp.clip(gz - 2 + i, 0, t4 - 1) + 1
        for j in range(8):
            x = jnp.clip(2 * gx - 3 + j, 0, x4 - 1) + 1
            k4[t, x, pl.ds(YO, y4), :] = smooth(q4, t, x, YO, y4)

    def up_c4(i):
        t = jnp.clip(gz - 1 + i, 0, t4 - 1) + 1
        for j in range(6):
            x = jnp.clip(2 * gx - 2 + j, 0, x4 - 1) + 1
            c4[t, x + 1, pl.ds(YO, y4), :] = solved(f4, h4, r4, k4, t, x, y4, 4)

    loop(5, up_k4, step=5)
    loop(3, up_c4, step=3)

    wait(m_w3)

    def spread_3(j):
        for i in range(6):
            value = c4[gz + j, 2 * gx + i, pl.ds(YO - 2 + 2 * gy, 6), :]
            prolong(q3, value, 1 + 2 * j, 2 * i, 0, 6)

    loop(3, spread_3, step=3)
    mask_k3, mask_c3 = row_mask(10, 3, 4), row_mask(8, 2, 4)

    def up_k3(i):
        mask = mask_k3 * tile_side(i - 2, 2)
        for x in range(-3, 7):
            v = smooth(q3, i + 1, x + 4, 1, 10)
            k3[i + 1, x + 4, pl.ds(1, 10), :] = masked(v, mask, side(0, x, 4))

    loop(6, up_k3, step=6)

    def up_c3(i):
        mask = mask_c3 * tile_side(i - 1, 2)
        for x in range(-2, 6):
            v = w3[i, x + 2, pl.ds(0, 8), :] + smooth(k3, i + 2, x + 4, 2, 8)
            prolong(q2, masked(v, mask, side(0, x, 4)), 2 * i + 1, 2 * x + 4, 0, 8)

    loop(4, up_c3, step=4)

    wait(m_w2)
    mask_k2, mask_c2 = row_mask(12, 2, 8), row_mask(10, 1, 8)

    def up_k2(i):
        mask = mask_k2 * tile_side(i - 1, 4)
        for x in range(-2, 10):
            v = smooth(q2, i + 2, x + 4, 2, 12)
            k2[i + 2, x + 4, pl.ds(2, 12), :] = masked(v, mask, side(0, x, 8))

    loop(6, up_k2, step=3)

    def up_c2(i):
        mask = mask_c2 * tile_side(i - 1, 4)
        for x in range(-1, 9):
            v = w2[i, x + 1, pl.ds(0, 10), :] + smooth(k2, i + 2, x + 4, 3, 10)
            prolong(q1, masked(v, mask, side(0, x, 8)), 2 * i, 2 * x + 2, 0, 10)

    loop(6, up_c2, step=3)

    mask = row_mask(18, 1, 16)

    def own_tile(t):
        for x in range(-1, 17):
            v = smooth(q1, t + 2, x + 2, 1, 18)
            k1[t + 2, x + 2, pl.ds(1, 18), :] = masked(v, mask, side(0, x, 16))

    def rim_tile(i):
        for x in range(16):
            v = smooth(q1, 9 * i + 1, x + 2, 2, 16)
            k1[9 * i + 1, x + 2, pl.ds(2, 16), :] = v * jnp.where(i > 0, inside[2][1], inside[2][0])

    loop(2, rim_tile, 2)
    loop(8, own_tile, step=2)

    def last(t):
        for x in range(16):
            v = w1[t, x] + smooth(k1, t + 2, x + 2, 2, 16)
            pot[x, :, pl.ds(pl.multiple_of(t * LANES, LANES), LANES)] = v

    loop(8, last, step=2)
    in_f4, in_h4, in_r4 = (cells(a, (t4, x4, y4), (1, 1, YO)) for a in (f4, h4, r4))
    energy(in_f4, lambda t, n: (in_f4(t, n) + in_h4(t, n)) * tau(4), (t4, x4, y4), 4, acc4)
    energy(in_h4, lambda t, n: (in_h4(t, n) + in_r4(t, n)) * tau(4), (t4, x4, y4), 4, acc4)
    in_f5, in_c5 = (cells(a, (t5, x5, y5), (1, 1, YO)) for a in (f5, c5))
    energy(in_f5, in_c5, (t5, x5, y5), 5, acc4)
    coarse_part = acc4[0:PAIRS, :] + swap(acc4[PAIRS:, :])
    wait(m_cc)
    packed = jnp.concatenate([cc[k] for k in range(ngz)], axis=0)
    scale = 4.0 / (ngx * ngy * ngz * 16 * 16 * 16)
    coul[0:32, :] = ((packed + coarse_part[0:32, :]) * scale)[:, :PAIRS]
    coul[32:64, :] = ((swap(packed) + coarse_part[32:64, :]) * scale)[:, :PAIRS]

    drain(tuple(sent))


def local(nums, density):
    ngx, ngy, ngz = nums
    piece = 32 // ngz

    def field(t, x, y):
        return pltpu.VMEM((t, x, y, LANES), F32)

    def level(t, x, y):
        return field(t + 2, x + 2, YO + -(-(y + 1) // 8) * 8)

    t4, x4, y4 = ngz, 2 * ngx, 2 * ngy
    l1, l2, l3 = level(8, 16, 16), level(4, 8, 8), level(2, 4, 4)
    e1, e2, e3 = field(12, 20, 32), field(8, 12, 24), field(6, 8, 16)
    l4, l5, l6 = (level(t4 // s, x4 // s, y4 // s) for s in (1, 2, 4))
    e6 = level(t4 // 2, x4 // 4, y4 // 4)
    c4 = field(t4 + 2, x4 + 4, 24)
    scratch = [e1, l1, l1, field(8, 16, 16), e2, l2, l2, field(6, 10, 16), e3, l3, l3, field(4, 8, 8)]
    scratch += [l4, l4, l4, l4, l4, c4, l5, l5, l5, l5, l5, l5, l6, e6, e6, e6]
    scratch += [field(8, 12, 16), field(8, 12, 16), field(1, 1, 8), field(10, 16, 16), field(10, 16, 16), field(1, 1, 8)]
    scratch += [field(12, 20, 24), field(12, 20, 24), field(8, 16, 16)]
    square = pltpu.VMEM((LANES, LANES), F32)
    row = pltpu.VMEM((piece, LANES), F32)
    scratch += [square, square, pltpu.VMEM((ngz, piece, LANES), F32), pltpu.VMEM((ngz, piece, LANES), F32), row]
    scratch += [pltpu.VMEM((ngx * ngy, piece, LANES), F32), row, pltpu.VMEM((ngz, piece, LANES), F32)]
    messages = 3 * (18 + 6) + 18 + 26 + 3 * (ngz - 1) + (ngx // 2 * ngy - 1) + (ngx * ngy - 1) + ngx // 2
    scratch += [pltpu.SemaphoreType.DMA((messages,)), pltpu.SemaphoreType.DMA((messages,)), pltpu.SemaphoreType.DMA((8,))]
    return pl.pallas_call(
        functools.partial(kernel, nums),
        out_shape=(pltpu.VMEM(density.shape, F32), pltpu.VMEM((PAIRS, PAIRS), F32)),
        in_specs=[pl.BlockSpec(memory_space=pl.ANY)],
        out_specs=(pl.BlockSpec(memory_space=pltpu.VMEM), pl.BlockSpec(memory_space=pltpu.VMEM)),
        scratch_shapes=scratch,
        compiler_params=pltpu.CompilerParams(
            collective_id=0, has_side_effects=True, vmem_limit_bytes=65_400_000
        ),
        name="cycle",
    )(density)


def solution(mesh):
    nums = tuple(mesh.shape[a] for a in ("gx", "gy", "gz"))
    placed = P("gx", "gy", "gz")
    return jax.shard_map(
        functools.partial(local, nums), mesh=mesh, in_specs=(placed,), out_specs=(placed, P()), check_vma=False
    )
```
